32 devices in a mesh: stage: 1 (over z), data: 32 (over y, x, core).
Axes of the slice: x: 4, y: 4, z: 1, core: 2. Of those that a mesh axis runs over, the one named last changes fastest.
The devices are a block of a 4x4x8 slice.
Arguments:
- grad_attn: float32 [32, 1, 2048, 2048], P(('stage', 'data'))
- mom_attn: float32 [1, 2048, 2048], P('stage', 'data')
- master_attn: float32 [1, 2048, 2048], P('stage', 'data')
- grad_up: float32 [32, 1, 2048, 1024], P(('stage', 'data'))
- mom_up: float32 [1, 2048, 1024], P('stage', 'data')
- master_up: float32 [1, 2048, 1024], P('stage', 'data')
- grad_down: float32 [32, 1, 1024, 2048], P(('stage', 'data'))
- mom_down: float32 [1, 1024, 2048], P('stage', 'data')
- master_down: float32 [1, 1024, 2048], P('stage', 'data')
Outputs:
- output 1: float32 [1, 2048, 2048], P('stage', 'data')
- output 2: float32 [1, 2048, 2048], P('stage', 'data')
- output 3: bfloat16 [1, 2048, 2048], P('stage', 'data')
- output 4: float32 [1, 2048, 1024], P('stage', 'data')
- output 5: float32 [1, 2048, 1024], P('stage', 'data')
- output 6: bfloat16 [1, 2048, 1024], P('stage', 'data')
- output 7: float32 [1, 1024, 2048], P('stage', 'data')
- output 8: float32 [1, 1024, 2048], P('stage', 'data')
- output 9: bfloat16 [1, 1024, 2048], P('stage', 'data')
All inputs are finite; a program needn't handle non-finite values.
Results may differ from the reference program's by a relative error of at most 0.0070479.
Values are sent between devices in bfloat16 or wider.
A program may use at most 768 MiB of HBM per device.

```python
import math
import jax
import jax.numpy as jnp
from jax import lax

HIDDEN = 2048
FFN_WIDTH = 1024
ATTN_COUNT = 1
EXPERT_COUNT = 1
GROUP_SIZE = 32
NS_STEPS = 5

MOMENTUM = 0.95
LEARN_RATE = 0.25
WEIGHT_DECAY = 0.2
EPSILON = 1e-7
COEF_A = 3.4445
COEF_B = -4.7750
COEF_C = 2.0315
STACK_SHAPES = ((ATTN_COUNT, HIDDEN, HIDDEN), (EXPERT_COUNT, HIDDEN, FFN_WIDTH), (EXPERT_COUNT, FFN_WIDTH, HIDDEN))
STACK_NAMES = ('attn', 'up', 'down')


def draw_grads(key, count, n_rows, n_cols):
    noise = jax.random.normal(key, (GROUP_SIZE, count, n_rows, n_cols), jnp.float32)
    row_owner = jnp.arange(n_rows) // (n_rows // GROUP_SIZE)
    scale = jnp.where(row_owner[None, :] == jnp.arange(GROUP_SIZE)[:, None], 0.8 * GROUP_SIZE, 0.5)
    return noise * scale[:, None, :, None]


def setup_inputs(seed: int = 0, part: int = 0) -> dict:
    base_key = jax.random.fold_in(jax.random.key(seed), part)
    keys = jax.random.split(base_key, 9)
    inputs = {}
    for stack_idx in range(3):
        count, n_rows, n_cols = STACK_SHAPES[stack_idx]
        label = STACK_NAMES[stack_idx]
        inputs['grad_' + label] = draw_grads(keys[3 * stack_idx], count, n_rows, n_cols)
        inputs['mom_' + label] = jax.random.normal(keys[3 * stack_idx + 1], (count, n_rows, n_cols), jnp.float32)
        inputs['master_' + label] = 0.5 * jax.random.normal(keys[3 * stack_idx + 2], (count, n_rows, n_cols), jnp.float32)
    return inputs


def orthogonalize(mom_new):
    n_rows, n_cols = mom_new.shape
    norm = jnp.sqrt(jnp.sum(mom_new * mom_new))
    x_mat = (mom_new / (norm + EPSILON)).astype(jnp.bfloat16)
    if n_rows > n_cols:
        x_mat = x_mat.T
    for _ in range(NS_STEPS):
        gram_mat = jnp.dot(x_mat, x_mat.T, preferred_element_type=jnp.float32).astype(jnp.bfloat16)
        gram_sq = jnp.dot(gram_mat, gram_mat, preferred_element_type=jnp.float32).astype(jnp.bfloat16)
        poly_mat = (COEF_B * gram_mat.astype(jnp.float32) + COEF_C * gram_sq.astype(jnp.float32)).astype(jnp.bfloat16)
        update = jnp.dot(poly_mat, x_mat, preferred_element_type=jnp.float32).astype(jnp.bfloat16)
        x_mat = (COEF_A * x_mat.astype(jnp.float32) + update.astype(jnp.float32)).astype(jnp.bfloat16)
    if n_rows > n_cols:
        x_mat = x_mat.T
    return x_mat


def stack_step(grad_all, mom_old, master_old):
    n_rows, n_cols = mom_old.shape[1], mom_old.shape[2]
    grad_mean = jnp.sum(grad_all, axis=0) / GROUP_SIZE
    mom_new = MOMENTUM * mom_old + grad_mean
    ortho_mat = lax.map(orthogonalize, mom_new)
    scale = 0.2 * math.sqrt(max(n_rows, n_cols))
    master_new = master_old - LEARN_RATE * (scale * ortho_mat.astype(jnp.float32) + WEIGHT_DECAY * master_old)
    return mom_new, master_new, master_new.astype(jnp.bfloat16)


def reference(grad_attn, mom_attn, master_attn, grad_up, mom_up, master_up, grad_down, mom_down, master_down):
    attn_out = stack_step(grad_attn, mom_attn, master_attn)
    up_out = stack_step(grad_up, mom_up, master_up)
    down_out = stack_step(grad_down, mom_down, master_down)
    return (attn_out[0], attn_out[1], attn_out[2], up_out[0], up_out[1], up_out[2], down_out[0], down_out[1], down_out[2])
```

```python
import functools
import math

import jax
import jax.numpy as jnp
from jax import lax
from jax.experimental import pallas as pl
from jax.experimental.pallas import tpu as pltpu
from jax.sharding import PartitionSpec as P

MOMENTUM = 0.95
LEARN_RATE = 0.25
WEIGHT_DECAY = 0.2
EPSILON = 1e-7
COEF_A = 3.4445
COEF_B = -4.7750
COEF_C = 2.0315
NS_STEPS = 5
F32 = jnp.float32
BF16 = jnp.bfloat16
MESH = pl.DeviceIdType.MESH
VMEM_LIMIT = 66_000_000


def ns_kernel(n, ax, xa, xu, xd, wa, wu, wd, wa_n, wa_b, wu_n, wu_b, wd_n, wd_b,
              X, A, B, stage, obuf, oa, ou, od, load_sem, asend, arecv, bsend, brecv, xsend, xrecv, osend, orecv):
    me = lax.axis_index(ax)
    role = lax.rem(me, 4)
    base = me - role
    blk = n // 4
    half = n // 2

    def dev(k):
        return {ax: k}

    barrier = pltpu.get_barrier_semaphore()
    for step in range(1, 4):
        pl.semaphore_signal(barrier, inc=1, device_id=dev(base + lax.rem(role + step, 4)), device_id_type=MESH)
    pl.semaphore_wait(barrier, 3)

    def at(ref, i, j):
        return ref.at[pl.ds(pl.multiple_of(i * blk, blk), blk), pl.ds(pl.multiple_of(j * blk, blk), blk)]

    def rows(i, size=blk):
        return pl.ds(pl.multiple_of(i * size, size), size)

    def poly(a, q):
        return (COEF_B * a.astype(F32) + COEF_C * q.astype(BF16).astype(F32)).astype(BF16)

    def blend(x, y):
        return (COEF_A * x.astype(F32) + y.astype(BF16).astype(F32)).astype(BF16)

    def dot_nt(a, b):
        return lax.dot_general(a, b, (((1,), (1,)), ((), ())), preferred_element_type=F32)

    def dot(a, b):
        return jnp.dot(a, b, preferred_element_type=F32)

    @pl.when(role < 2)
    def _():
        c = role
        peer = dev(base + 1 - c)
        p_own, s_own = 3 * c, 1 + c
        p_peer, s_peer = 3 - 3 * c, 2 - c
        i1, j1 = 1 + 2 * c, 3 - 3 * c
        i2, j2 = 2 * c, 2 - c

        loads = [pltpu.make_async_copy(xa.at[rows(p)], X.at[0, rows(p)], load_sem.at[k])
                 for k, p in enumerate((p_own, s_own, p_peer, s_peer))]
        for cp in loads:
            cp.start()
        for cp in loads:
            cp.wait()

        def a_copy(k, i, j):
            return pltpu.make_async_remote_copy(at(A, i, j), at(A, i, j), asend.at[k], arecv.at[k],
                                                device_id=peer, device_id_type=MESH)

        a_blocks = ((p_own, p_own), (p_own, s_own), (s_own, p_own), (i1, j1), (j1, i1), (i2, j2), (j2, i2), (s_own, s_own))

        def a_send(k):
            a_copy(k, *a_blocks[k]).start()

        def a_wait(*ks):
            for k in ks:
                a_copy(k, *a_blocks[k]).wait_recv()

        def x_copy(nxt, p, j, k):
            ref = at(X.at[nxt], p, j)
            return pltpu.make_async_remote_copy(ref, ref, xsend.at[k, j], xrecv.at[k, j],
                                                device_id=peer, device_id_type=MESH)

        def x_wait(cur, k):
            for j in range(4):
                x_copy(cur, (p_peer, s_peer)[k], j, k).wait_recv()

        def b_copy(k):
            i, j = ((i1, j1), (i2, j2))[k]
            return pltpu.make_async_remote_copy(stage.at[k], at(B, j - 2 * (1 - c), i), bsend.at[k], brecv.at[k],
                                                device_id=peer, device_id_type=MESH)

        def gram(xt, i, j, mirror):
            v = dot_nt(xt[rows(i), :], xt[rows(j), :]).astype(BF16)
            at(A, i, j)[...] = v
            if mirror:
                at(A, j, i)[...] = v.T

        def a_step(t, cur):
            xt = X.at[cur]
            gram(xt, p_own, p_own, False)

            @pl.when(t > 0)
            def _():
                x_wait(cur, 0)
            a_send(0)
            gram(xt, p_own, s_own, True)
            a_send(1)
            a_send(2)
            gram(xt, i1, j1, True)
            a_send(3)
            a_send(4)

            @pl.when(t > 0)
            def _():
                x_wait(cur, 1)
            gram(xt, i2, j2, True)
            a_send(5)
            a_send(6)
            gram(xt, s_own, s_own, False)
            a_send(7)

        def x_wait_send(nxt):
            for k, p in enumerate((p_own, s_own)):
                for j in range(4):
                    x_copy(nxt, p, j, k).wait_send()

        def q_block(i, j):
            q = dot(A[rows(i), :], A[:, pl.ds(pl.multiple_of(j * blk, blk), blk)])
            v = poly(at(A, i, j)[...], q)
            at(B, i - 2 * c, j)[...] = v
            return v

        def q_step(t, cur):
            a_wait(3, 4)
            q_block(p_own, p_own)
            a_wait(5, 6)
            v = q_block(p_own, s_own)
            at(B, s_own - 2 * c, p_own)[...] = v.T
            a_wait(0, 1, 2)
            v = q_block(i1, j1)
            stage[0] = v.T
            b_copy(0).start()
            a_wait(7)
            v = q_block(i2, j2)
            stage[1] = v.T
            b_copy(1).start()
            q_block(s_own, s_own)
            for k in range(8):
                a_copy(k, *a_blocks[k]).wait_send()

            @pl.when(t > 0)
            def _():
                x_wait_send(cur)

        def y_step(cur, nxt):
            xt, xn = X.at[cur], X.at[nxt]
            for k, p in enumerate((p_own, s_own)):
                b_copy(k).wait_recv()

                @pl.loop(0, 4)
                def _(j):
                    cols = pl.ds(pl.multiple_of(j * blk, blk), blk)
                    y = dot(B[rows(p - 2 * c), :], xt[:, cols])
                    at(xn, p, j)[...] = blend(at(xt, p, j)[...], y)
                    x_copy(nxt, p, j, k).start()
            for k in range(2):
                b_copy(k).wait_send()

        @pl.loop(0, NS_STEPS - 1)
        def _(t):
            cur = lax.rem(t, 2)
            nxt = 1 - cur
            a_step(t, cur)
            q_step(t, cur)
            y_step(cur, nxt)

        last = NS_STEPS - 1
        cur = last % 2
        a_step(last, cur)
        a_wait(*range(8))
        for k in range(8):
            a_copy(k, *a_blocks[k]).wait_send()
        x_wait_send(cur)
        own = oa.shape[0]
        mine = pl.ds(pl.multiple_of(own * (base + 2 * c), 2 * own), 2 * own)
        for j in range(4):
            cols = pl.ds(j * blk, blk)
            B[0:2 * own, cols] = poly(A[mine, cols], dot(A[mine, :], A[:, cols]))
        for j in range(4):
            cols = pl.ds(j * blk, blk)
            obuf[0:2 * own, cols] = blend(X[cur, mine, cols], dot(B[0:2 * own, :], X[cur, :, cols]))

        def o_copy(k, target):
            return pltpu.make_async_remote_copy(obuf.at[pl.ds(own * k, own)], oa, osend.at[k], orecv.at[0],
                                                device_id=dev(target), device_id_type=MESH)

        @pl.when(c == 1)
        def _():
            o_copy(0, base + 2).start()
            o_copy(1, base + 3).start()
            o_copy(0, base + 2).wait_send()
            o_copy(1, base + 3).wait_send()

        @pl.when(c == 0)
        def _():
            o_copy(1, base + 1).start()
            oa[...] = obuf[0:own, :]
            o_copy(1, base + 1).wait_send()

    @pl.when(role >= 2)
    def _():
        @pl.when(role == 2)
        def _():
            cp = pltpu.make_async_copy(xu, X.at[1, :, pl.ds(0, half)], load_sem.at[0])
            cp.start()
            cp.wait()

            @pl.loop(0, 4)
            def _(i):
                for j in range(2):
                    at(X.at[0], j, i)[...] = at(X.at[1], i, j)[...].T

        @pl.when(role == 3)
        def _():
            cp = pltpu.make_async_copy(xd, X.at[0, pl.ds(0, half)], load_sem.at[0])
            cp.start()
            cp.wait()

        def a_step(cur):
            @pl.loop(0, 2)
            def _(i):
                for j in range(2):
                    at(A, i, j)[...] = dot_nt(X[cur, rows(i), :], X[cur, j * blk:(j + 1) * blk, :]).astype(BF16)

        def q_rows(i):
            for j in range(2):
                q = dot(A[rows(i), 0:half], A[0:half, j * blk:(j + 1) * blk])
                at(B, i, j)[...] = poly(at(A, i, j)[...], q)

        @pl.loop(0, NS_STEPS - 1)
        def _(t):
            cur = lax.rem(t, 2)
            nxt = 1 - cur
            a_step(cur)

            @pl.loop(0, 2)
            def _(i):
                q_rows(i)

            @pl.loop(0, 4)
            def _(j):
                cols = pl.ds(pl.multiple_of(j * blk, blk), blk)
                for i in range(2):
                    y = dot(B[i * blk:(i + 1) * blk, 0:half], X[cur, 0:half, cols])
                    at(X.at[nxt], i, j)[...] = blend(at(X.at[cur], i, j)[...], y)

        cur = (NS_STEPS - 1) % 2
        a_step(cur)

        @pl.when(role == 2)
        def _():
            own = ou.shape[0]
            cols = pl.ds(pl.multiple_of(own * base, 4 * own), 4 * own)
            for i in range(2):
                q_rows(i)
            for i in range(2):
                o = blend(X[cur, i * blk:(i + 1) * blk, cols], dot(B[i * blk:(i + 1) * blk, 0:half], X[cur, 0:half, cols]))
                obuf[0:4 * own, i * blk:(i + 1) * blk] = o.T

            def o_copy(k):
                return pltpu.make_async_remote_copy(obuf.at[pl.ds(own * k, own), pl.ds(0, half)], ou, osend.at[k], orecv.at[1],
                                                    device_id=dev(base + k), device_id_type=MESH)
            for k in (0, 1, 3):
                o_copy(k).start()
            ou[...] = obuf[2 * own:3 * own, 0:half]
            for k in (0, 1, 3):
                o_copy(k).wait_send()

        @pl.when(role == 3)
        def _():
            own = od.shape[0]
            mine = pl.ds(pl.multiple_of(own * base, 4 * own), 4 * own)
            for j in range(2):
                cols = pl.ds(j * blk, blk)
                B[0:4 * own, cols] = poly(A[mine, cols], dot(A[mine, 0:half], A[0:half, cols]))
            for j in range(4):
                cols = pl.ds(j * blk, blk)
                obuf[0:4 * own, cols] = blend(X[cur, mine, cols], dot(B[0:4 * own, 0:half], X[cur, 0:half, cols]))

            def o_copy(k):
                return pltpu.make_async_remote_copy(obuf.at[pl.ds(own * k, own)], od, osend.at[k], orecv.at[2],
                                                    device_id=dev(base + k), device_id_type=MESH)
            for k in (0, 1, 2):
                o_copy(k).start()
            od[...] = obuf[3 * own:4 * own, :]
            for k in (0, 1, 2):
                o_copy(k).wait_send()

    def update(o, w, w_n, w_b, scale):
        old = w[...]
        new = old - LEARN_RATE * (scale * o[...].astype(F32) + WEIGHT_DECAY * old)
        w_n[...] = new
        w_b[...] = new.astype(BF16)

    def arrived(o, k):
        pltpu.make_async_remote_copy(o, o, osend.at[k], orecv.at[k], device_id=dev(base), device_id_type=MESH).wait_recv()

    scale = 0.2 * math.sqrt(n)

    @pl.when(role != 3)
    def _():
        arrived(od, 2)
    update(od, wd, wd_n, wd_b, scale)

    @pl.when(role != 2)
    def _():
        arrived(ou, 1)
    update(ou, wu, wu_n, wu_b, scale)

    @pl.when(role != 0)
    def _():
        arrived(oa, 0)
    update(oa, wa, wa_n, wa_b, scale)


def orthogonalize(ax, xa, xu, xd, wa, wu, wd):
    n = xa.shape[1]
    blk = n // 4
    dma = pltpu.SemaphoreType.DMA
    vmem = pl.BlockSpec(memory_space=pltpu.VMEM)
    hbm = pl.BlockSpec(memory_space=pl.ANY)
    outs = []
    for w in (wa, wu, wd):
        outs += [jax.ShapeDtypeStruct(w.shape, F32), jax.ShapeDtypeStruct(w.shape, BF16)]
    return pl.pallas_call(
        functools.partial(ns_kernel, n, ax),
        name="newton_schulz",
        out_shape=outs,
        in_specs=[hbm] * 3 + [vmem] * 3,
        out_specs=[vmem] * 6,
        scratch_shapes=[
            pltpu.VMEM((2, n, n), BF16),
            pltpu.VMEM((n, n), BF16),
            pltpu.VMEM((n // 2, n), BF16),
            pltpu.VMEM((2, blk, blk), BF16),
            pltpu.VMEM((4 * max(wa.shape[0], wu.shape[0]), n), BF16),
            pltpu.VMEM(wa.shape, BF16),
            pltpu.VMEM(wu.shape, BF16),
            pltpu.VMEM(wd.shape, BF16),
            dma((4,)), dma((8,)), dma((8,)), dma((2,)), dma((2,)), dma((2, 4)), dma((2, 4)), dma((4,)), dma((3,)),
        ],
        compiler_params=pltpu.CompilerParams(collective_id=1, has_side_effects=True, vmem_limit_bytes=VMEM_LIMIT),
    )(xa, xu, xd, wa, wu, wd)


def solution(mesh):
    ax = mesh.axis_names[1]
    group = mesh.shape[ax]
    grad_spec = P(tuple(mesh.axis_names), None, None, None)
    row_spec = P(mesh.axis_names[0], ax, None)

    def step_local(*arrays):
        moms, gathered, masters = [], [], []
        for k in range(3):
            grad, mom, master = arrays[3 * k:3 * k + 3]
            grad_rows = lax.psum_scatter(grad[0, 0], ax, scatter_dimension=0, tiled=True) / group
            mom_new = MOMENTUM * mom[0] + grad_rows
            norm_sq = lax.psum(jnp.sum(mom_new * mom_new), ax)
            x_rows = (mom_new / (jnp.sqrt(norm_sq) + EPSILON)).astype(BF16)
            moms.append(mom_new)
            gathered.append(lax.all_gather(x_rows, ax, axis=0, tiled=True))
            masters.append(master[0])
        new = orthogonalize(ax, *gathered, *masters)
        results = []
        for k in range(3):
            results += [moms[k][None], new[2 * k][None], new[2 * k + 1][None]]
        return tuple(results)

    return jax.shard_map(step_local, mesh=mesh, in_specs=(grad_spec, row_spec, row_spec) * 3,
                         out_specs=(row_spec,) * 9, check_vma=False)
```

```python
import functools
import math

import jax
import jax.numpy as jnp
from jax import lax
from jax.experimental import pallas as pl
from jax.experimental.pallas import tpu as pltpu
from jax.sharding import PartitionSpec as P

MOMENTUM = 0.95
LEARN_RATE = 0.25
WEIGHT_DECAY = 0.2
EPSILON = 1e-7
COEF_A = 3.4445
COEF_B = -4.7750
COEF_C = 2.0315
NS_STEPS = 5
F32 = jnp.float32
BF16 = jnp.bfloat16
MESH = pl.DeviceIdType.MESH
VMEM_LIMIT = 66_000_000
ATTN, UP, DOWN = MATRICES = range(3)
FIRST, SECOND = PAIR = range(2)
ALL = slice(None)
QUAD = range(4)


class Comm:
    def __init__(self, side, group, ax, mats, slots, local_sem, send_sem, recv_sem):
        self.side, self.group, self.ax, self.mats, self.slots = side, group, ax, mats, slots
        self.local_sem, self.send_sem, self.recv_sem = local_sem, send_sem, recv_sem
        me = lax.axis_index(ax)
        self.role = lax.rem(me, 4)
        self.c = lax.rem(me, 2)
        self.x = lax.rem(me // 2, side)
        self.y = me // (2 * side)
        self.peer = self.dev(self.y, self.x, 1 - self.c)
        self.pos = ((self.x, self.y), (self.y, self.x))
        self.keys, self.local_keys, self.sent, self.peer_only = {}, {}, {}, {}

    def dev(self, yy, xx, cc):
        return {self.ax: (lax.rem(yy, self.side) * self.side + lax.rem(xx, self.side)) * 2 + cc}

    def greet(self):
        barrier = pltpu.get_barrier_semaphore()
        pl.semaphore_signal(barrier, inc=1, device_id=self.peer, device_id_type=MESH)
        for k in range(1, self.side):
            pl.semaphore_signal(barrier, inc=1, device_id=self.dev(self.y + k, self.x, self.c), device_id_type=MESH)
            pl.semaphore_signal(barrier, inc=1, device_id=self.dev(self.y, self.x + k, self.c), device_id_type=MESH)
        return 2 * self.side - 1

    def to(self, along_x, step):
        step = step % self.side
        return self.dev(self.y, self.x + step, self.c) if along_x else self.dev(self.y + step, self.x, self.c)

    def remote(self, key, src, dst, target):
        k = self.keys.setdefault(key, len(self.keys))
        return pltpu.make_async_remote_copy(src, dst, self.send_sem.at[k], self.recv_sem.at[k],
                                            device_id=target, device_id_type=MESH)

    def local(self, key, src, dst):
        k = self.local_keys.setdefault(key, len(self.local_keys))
        return pltpu.make_async_copy(src, dst, self.local_sem.at[k])

    def start(self, make, *args):
        make(*args).start()
        self.sent[(make.__name__,) + args] = (make, args)

    def finish(self):
        for make, args in self.sent.values():
            make(*args).wait_send()

    def shift(self, p, k):
        return lax.rem(p + k, self.side)

    def quarter(self, m, f, h):
        q = self.mats[m]["own"].shape[-1] // 4
        return pl.ds((2 * f + h) * q, q)

    def half(self, m, f):
        q = self.mats[m]["own"].shape[-1] // 2
        return pl.ds(f * q, q)

    @staticmethod
    def lane1(f, k):
        return (ALL, k) if f == 0 else (k, ALL)

    def lane2(self, f, k):
        return (k, self.x) if f == 0 else (self.y, k)

    @staticmethod
    def one(f, k, i):
        return (i, k) if f == 0 else (k, i)

    def pair_remote(self, m, f, k):
        idx = self.lane1(f, self.shift(self.pos[f][0], k))
        cols = self.half(m, f)
        mat = self.mats[m]
        return self.remote(("pair", m, f, k), mat["grad"].at[idx + (1 - self.c, ALL, cols)],
                           mat["peer"].at[idx + (ALL, cols)], self.peer)

    def pair_local(self, m, f, k):
        idx = self.lane1(f, self.shift(self.pos[f][0], k))
        cols = self.half(m, f)
        mat = self.mats[m]
        return self.local(("pair", m, f, k), mat["grad"].at[idx + (self.c, ALL, cols)],
                          mat["sum"].at[idx + (ALL, cols)])

    def pair_start(self, m):
        for k in (2, 1, self.side - 1, 0):
            for f in PAIR:
                self.start(self.pair_remote, m, f, k)
                self.pair_local(m, f, k).start()

    def pair_sum(self, m, f, k):
        self.pair_remote(m, f, k).wait_recv()
        self.pair_local(m, f, k).wait()
        kk = self.shift(self.pos[f][0], k)
        cols = self.half(m, f)
        total, other = self.mats[m]["sum"], self.mats[m]["peer"]

        @pl.loop(0, self.side)
        def _(i):
            idx = self.one(f, kk, i) + (ALL, cols)
            total[idx] = total[idx] + other[idx]

    def ring(self, m, f, phase, j):
        k, h, step = ((2, 1, 1), (2, 0, -1), (1, 0, 1), (-1, 1, -1), (1, 1, 1), (-1, 0, -1))[j]
        kk = self.shift(self.pos[f][phase], k % self.side)
        idx = (self.lane1, self.lane2)[phase](f, kk) + (ALL, self.quarter(m, f, h))
        mat = self.mats[m]
        return self.remote(("ring", m, f, phase, j), mat["sum"].at[idx], mat[("ring1", "ring2")[phase]].at[f, j],
                           self.to((f == 0) == (phase == 0), step))

    def ring_add(self, m, f, phase, j, k, h):
        self.ring(m, f, phase, j).wait_recv()
        kk = self.shift(self.pos[f][phase], k % self.side)
        cols = self.quarter(m, f, h)
        mat = self.mats[m]
        total = mat["sum"]
        if phase == 0:
            @pl.loop(0, self.side)
            def _(i):
                idx = self.one(f, kk, i) + (ALL, cols)
                total[idx] = total[idx] + mat["ring1"][f, j, i]
        else:
            idx = self.lane2(f, kk) + (ALL, cols)
            total[idx] = total[idx] + mat["ring2"][f, j]

    def rs_far(self, m):
        for f in PAIR:
            self.pair_sum(m, f, 2)
            self.start(self.ring, m, f, 0, 0)
            self.start(self.ring, m, f, 0, 1)

    def rs_near(self, m):
        for f in PAIR:
            self.pair_sum(m, f, 1)
            self.start(self.ring, m, f, 0, 2)
            self.pair_sum(m, f, self.side - 1)
            self.start(self.ring, m, f, 0, 3)

    def rs_own(self, m):
        for f in PAIR:
            self.pair_sum(m, f, 0)

    def pass_on(self, m, phase):
        for f in PAIR:
            self.ring_add(m, f, phase, 0, 1, 1)
            self.start(self.ring, m, f, phase, 4)
            self.ring_add(m, f, phase, 1, -1, 0)
            self.start(self.ring, m, f, phase, 5)

    def settle(self, m, phase):
        for f in PAIR:
            for j, h in ((2, 0), (3, 1), (4, 1), (5, 0)):
                self.ring_add(m, f, phase, j, 0, h)
            if phase == 0:
                for j in range(4):
                    self.start(self.ring, m, f, 1, j)

    def norm_pair(self, m):
        ref = self.slots.at[m, 0, self.c]
        return self.remote(("norm", m), ref, ref, self.peer)

    def norm_line(self, m, level, k):
        ref = self.slots.at[m, level, self.x if level == 1 else self.y]
        return self.remote(("norm", m, level, k), ref, ref, self.to(level == 1, k))

    def momentum(self, m):
        mat = self.mats[m]
        rows, cols = mat["mom"].shape
        mat["new"][...] = MOMENTUM * mat["mom"][...] + mat["sum"][self.y, self.x] / self.group
        acc = jnp.zeros((8, 128), F32)
        for i in range(0, rows, 8):
            for j in range(0, cols, 128):
                part = mat["new"][i:i + 8, j:j + 128]
                acc = acc + part * part
        self.slots[m, 0, self.c] = acc
        self.start(self.norm_pair, m)

    def norm_x(self, m):
        self.norm_pair(m).wait_recv()
        self.slots[m, 1, self.x] = self.slots[m, 0, 0] + self.slots[m, 0, 1]
        for k in range(1, self.side):
            self.start(self.norm_line, m, 1, k)

    def level_sum(self, m, level):
        for k in range(1, self.side):
            self.norm_line(m, level, k).wait_recv()
        acc = self.slots[m, level, 0]
        for k in range(1, self.side):
            acc = acc + self.slots[m, level, k]
        return acc

    def norm_y(self, m):
        self.slots[m, 2, self.y] = self.level_sum(m, 1)
        for k in range(1, self.side):
            self.start(self.norm_line, m, 2, k)

    def normalize(self, m):
        mat = self.mats[m]
        norm = jnp.sqrt(jnp.sum(self.level_sum(m, 2), axis=(0, 1), keepdims=True))
        mat["own"][...] = (mat["new"][...] / (norm + EPSILON)).astype(BF16)

    def along(self, f, phase):
        return (f == 0) != (phase == 0)

    def gpos(self, f, phase):
        return self.x if self.along(f, phase) else self.y

    def spot(self, m, f, phase, k, cols):
        if phase == 0:
            idx = (k, self.x) if f == 0 else (self.y, k)
        else:
            idx = self.lane1(f, k)
        return self.mats[m]["full"].at[idx + (self.c, ALL, cols)]

    def ag_own(self, m):
        return self.local(("own", m), self.mats[m]["own"], self.mats[m]["full"].at[self.y, self.x, self.c])

    def ag_send(self, m, f, phase, j):
        dst = self.spot(m, f, phase, self.gpos(f, phase), self.half(m, f))
        src = self.mats[m]["own"].at[:, self.half(m, f)] if phase == 0 else dst
        return self.remote(("send", m, f, phase, j), src, dst, self.to(self.along(f, phase), (1, -1)[j]))

    def ag_relay(self, m, f, phase, j):
        ref = self.spot(m, f, phase, self.shift(self.gpos(f, phase), (self.side - 1, 1)[j]), self.quarter(m, f, (1, 0)[j]))
        return self.remote(("relay", m, f, phase, j), ref, ref, self.to(self.along(f, phase), (1, -1)[j]))

    def ag_peer(self, m, f, k):
        ref = self.spot(m, f, 1, self.shift(self.gpos(f, 1), k), self.half(m, f))
        return self.remote(("peer", m, f, k), ref, ref, self.peer)

    def to_peer(self, m, f, k):
        self.peer_only[m, f, k] = True

        @pl.when(self.sends(m))
        def _():
            self.ag_peer(m, f, k).start()

    def sends(self, m):
        return self.role < 2 if m == 0 else self.role == 4 - m

    def needs(self, m):
        return self.role < 2 if m == 0 else self.role == 1 + m

    def ag_start(self, m):
        self.ag_own(m).start()
        for f in PAIR:
            for j in PAIR:
                self.start(self.ag_send, m, f, 0, j)

    def ag_forward(self, m, phase):
        for f in PAIR:
            for j in PAIR:
                self.ag_send(m, f, phase, j).wait_recv()
                self.start(self.ag_relay, m, f, phase, j)
                if phase == 1:
                    self.to_peer(m, f, (self.side - 1, 1)[j])

    def ag_turn(self, m):
        self.ag_own(m).wait()
        for f in PAIR:
            for j in PAIR:
                self.ag_relay(m, f, 0, j).wait_recv()
            for j in PAIR:
                self.start(self.ag_send, m, f, 1, j)
            self.to_peer(m, f, 0)

    def ag_end(self, m):
        for f in PAIR:
            for j in PAIR:
                self.ag_relay(m, f, 1, j).wait_recv()
            self.to_peer(m, f, 2)

    def ag_arrived(self, m):
        @pl.when(self.needs(m))
        def _():
            for f in PAIR:
                for k in range(self.side):
                    self.ag_peer(m, f, k).wait_recv()

    def ag_finish(self, m):
        @pl.when(self.sends(m))
        def _():
            for f in PAIR:
                for k in range(self.side):
                    self.ag_peer(m, f, k).wait_send()


def reduce_kernel(side, group, ax, ga, gu, ma, mu, na, nu, xu, xa,
                  sa, su, pa, pu, ra1, ru1, ra2, ru2, xra, slots, local_sem, send_sem, recv_sem):
    mats = {0: dict(grad=ga, mom=ma, new=na, full=xa, sum=sa, peer=pa, ring1=ra1, ring2=ra2, own=xra),
            1: dict(grad=gu, mom=mu, new=nu, sum=su, peer=pu, ring1=ru1, ring2=ru2, own=xu)}
    comm = Comm(side, group, ax, mats, slots, local_sem, send_sem, recv_sem)
    pl.semaphore_wait(pltpu.get_barrier_semaphore(), comm.greet())
    comm.pair_start(ATTN)
    comm.pair_start(UP)
    comm.rs_far(ATTN)
    comm.rs_near(ATTN)
    comm.rs_own(ATTN)
    comm.pass_on(ATTN, FIRST)
    comm.settle(ATTN, FIRST)
    comm.pass_on(ATTN, SECOND)
    comm.rs_far(UP)
    comm.settle(ATTN, SECOND)
    comm.momentum(ATTN)
    comm.rs_near(UP)
    comm.norm_x(ATTN)
    comm.rs_own(UP)
    comm.norm_y(ATTN)
    comm.normalize(ATTN)
    comm.ag_start(ATTN)
    comm.pass_on(UP, FIRST)
    comm.ag_forward(ATTN, FIRST)
    comm.ag_turn(ATTN)
    comm.settle(UP, FIRST)
    comm.pass_on(UP, SECOND)
    comm.ag_forward(ATTN, SECOND)
    comm.settle(UP, SECOND)
    comm.momentum(UP)
    comm.norm_x(UP)
    comm.norm_y(UP)
    comm.normalize(UP)
    comm.ag_end(ATTN)
    comm.ag_arrived(ATTN)
    comm.finish()
    comm.ag_finish(ATTN)


def scratch_for(side, shapes):
    scratch = [pltpu.VMEM((side, side) + s, F32) for s in shapes] * 2
    scratch += [pltpu.VMEM((2, 6, side, s[0], s[1] // 4), F32) for s in shapes]
    scratch += [pltpu.VMEM((2, 6, s[0], s[1] // 4), F32) for s in shapes]
    return scratch


def reduce_and_gather(side, ax, grads, moms):
    dma = pltpu.SemaphoreType.DMA
    vmem = pl.BlockSpec(memory_space=pltpu.VMEM)
    hbm = pl.BlockSpec(memory_space=pl.ANY)
    group = 2 * side * side
    shapes = [m.shape for m in moms]
    views = [g.reshape(side, side, 2, *s) for g, s in zip(grads, shapes)]
    scratch = scratch_for(side, shapes) + [pltpu.VMEM(shapes[0], BF16)]
    scratch += [pltpu.VMEM((2, 3, side, 8, 128), F32), dma((20,)), dma((110,)), dma((110,))]
    na, nu, xu, xa = pl.pallas_call(
        functools.partial(reduce_kernel, side, group, ax),
        name="reduce_gather",
        out_shape=[jax.ShapeDtypeStruct(s, F32) for s in shapes]
        + [jax.ShapeDtypeStruct(shapes[1], BF16), jax.ShapeDtypeStruct((side, side, 2) + shapes[0], BF16)],
        in_specs=[hbm] * 2 + [vmem] * 2,
        out_specs=[vmem] * 3 + [hbm],
        scratch_shapes=scratch,
        compiler_params=pltpu.CompilerParams(collective_id=0, has_side_effects=True, vmem_limit_bytes=VMEM_LIMIT),
    )(*views, *moms)
    return na, nu, xu, xa.reshape(group * shapes[0][0], shapes[0][1])


def ns_kernel(n, side, group, ax, xa, xur, gd, md, oa_out, ou_out, od_out, nd, xu, xd,
              X, A, B, stage, obuf, oa, ou, od, sd, pd, rd1, rd2, xrd, slots,
              load_sem, asend, arecv, bsend, brecv, xsend, xrecv, osend, orecv, local_sem, send_sem, recv_sem):
    me = lax.axis_index(ax)
    role = lax.rem(me, 4)
    base = me - role
    mats = {1: dict(full=xu, own=xur),
            2: dict(grad=gd, mom=md, new=nd, full=xd, sum=sd, peer=pd, ring1=rd1, ring2=rd2, own=xrd)}
    comm = Comm(side, group, ax, mats, slots, local_sem, send_sem, recv_sem)
    blk = n // 4
    half = n // 2

    def dev(k):
        return {ax: k}

    barrier = pltpu.get_barrier_semaphore()
    greeted = comm.greet()
    for step in range(1, 4):
        pl.semaphore_signal(barrier, inc=1, device_id=dev(base + lax.rem(role + step, 4)), device_id_type=MESH)
    pl.semaphore_wait(barrier, greeted + 3)
    comm.pair_start(DOWN)
    comm.ag_start(UP)
    steps = (
        ("0A1", (comm.rs_far, DOWN)),
        ("0A2", (comm.rs_near, DOWN)),
        ("0A4", (comm.ag_forward, UP, FIRST)),
        ("0Q1", (comm.rs_own, DOWN), (comm.pass_on, DOWN, FIRST)),
        ("0Q3", (comm.ag_turn, UP)),
        ("0P2", (comm.settle, DOWN, FIRST)),
        ("0S1", (comm.pass_on, DOWN, SECOND)),
        ("1A0", (comm.settle, DOWN, SECOND), (comm.momentum, DOWN)),
        ("1A1", (comm.norm_x, DOWN)),
        ("1A3", (comm.norm_y, DOWN)),
        ("1Q0", (comm.normalize, DOWN), (comm.ag_start, DOWN)),
        ("1Q1", (comm.ag_forward, UP, SECOND)),
        ("1Q3", (comm.ag_forward, DOWN, FIRST)),
        ("1P1", (comm.ag_turn, DOWN)),
        ("1P3", (comm.ag_end, UP)),
        ("1S3", (comm.ag_forward, DOWN, SECOND)),
        ("2A2", (comm.ag_end, DOWN)),
    )

    def run(calls):
        for call, *what in calls:
            call(*what)

    def tick(t, part, i):
        if isinstance(t, int):
            return
        for (when, where, block), *calls in steps:
            if where == part:
                go = jnp.logical_and(t == int(when), i == int(block))
                pl.when(go)(functools.partial(run, calls))

    def at(ref, i, j):
        return ref.at[pl.ds(pl.multiple_of(i * blk, blk), blk), pl.ds(pl.multiple_of(j * blk, blk), blk)]

    def rows(i, size=blk):
        return pl.ds(pl.multiple_of(i * size, size), size)

    def poly(a, q):
        return (COEF_B * a.astype(F32) + COEF_C * q.astype(BF16).astype(F32)).astype(BF16)

    def blend(x, y):
        return (COEF_A * x.astype(F32) + y.astype(BF16).astype(F32)).astype(BF16)

    def dot_nt(a, b):
        return lax.dot_general(a, b, (((1,), (1,)), ((), ())), preferred_element_type=F32)

    def dot(a, b):
        return jnp.dot(a, b, preferred_element_type=F32)

    @pl.when(role < 2)
    def _():
        c = role
        peer = dev(base + 1 - c)
        p_own, s_own = 3 * c, 1 + c
        p_peer, s_peer = 3 - 3 * c, 2 - c
        i1, j1 = 1 + 2 * c, 3 - 3 * c
        i2, j2 = 2 * c, 2 - c

        loads = [pltpu.make_async_copy(xa.at[rows(p)], X.at[0, rows(p)], load_sem.at[k])
                 for k, p in enumerate((p_own, s_own, p_peer, s_peer))]
        for cp in loads:
            cp.start()
        for cp in loads:
            cp.wait()

        def a_copy(k, i, j):
            return pltpu.make_async_remote_copy(at(A, i, j), at(A, i, j), asend.at[k], arecv.at[k],
                                                device_id=peer, device_id_type=MESH)

        a_blocks = ((p_own, p_own), (p_own, s_own), (s_own, p_own), (i1, j1), (j1, i1), (i2, j2), (j2, i2), (s_own, s_own))
        PP, PS, SP, C1, T1, C2, T2, SS = every = range(len(a_blocks))

        def a_send(k):
            a_copy(k, *a_blocks[k]).start()

        def a_wait(*ks):
            for k in ks:
                a_copy(k, *a_blocks[k]).wait_recv()

        def x_copy(nxt, p, j, k):
            ref = at(X.at[nxt], p, j)
            return pltpu.make_async_remote_copy(ref, ref, xsend.at[k, j], xrecv.at[k, j],
                                                device_id=peer, device_id_type=MESH)

        def x_wait(cur, k):
            for j in QUAD:
                x_copy(cur, (p_peer, s_peer)[k], j, k).wait_recv()

        def b_copy(k):
            i, j = ((i1, j1), (i2, j2))[k]
            return pltpu.make_async_remote_copy(stage.at[k], at(B, j - 2 * (1 - c), i), bsend.at[k], brecv.at[k],
                                                device_id=peer, device_id_type=MESH)

        def gram(xt, i, j, mirror):
            v = dot_nt(xt[rows(i), :], xt[rows(j), :]).astype(BF16)
            at(A, i, j)[...] = v
            if mirror:
                at(A, j, i)[...] = v.T

        def a_step(t, cur):
            xt = X.at[cur]
            gram(xt, p_own, p_own, False)
            tick(t, "A", 0)

            @pl.when(t > 0)
            def _():
                x_wait(cur, FIRST)
            a_send(PP)
            gram(xt, p_own, s_own, True)
            a_send(PS)
            a_send(SP)
            tick(t, "A", 1)
            gram(xt, i1, j1, True)
            a_send(C1)
            a_send(T1)
            tick(t, "A", 2)

            @pl.when(t > 0)
            def _():
                x_wait(cur, SECOND)
            gram(xt, i2, j2, True)
            a_send(C2)
            a_send(T2)
            tick(t, "A", 3)
            gram(xt, s_own, s_own, False)
            a_send(SS)
            tick(t, "A", 4)

        def x_wait_send(nxt):
            for k, p in enumerate((p_own, s_own)):
                for j in QUAD:
                    x_copy(nxt, p, j, k).wait_send()

        def q_block(i, j):
            q = dot(A[rows(i), :], A[:, pl.ds(pl.multiple_of(j * blk, blk), blk)])
            v = poly(at(A, i, j)[...], q)
            at(B, i - 2 * c, j)[...] = v
            return v

        def q_step(t, cur):
            a_wait(C1, T1)
            q_block(p_own, p_own)
            tick(t, "Q", 0)
            a_wait(C2, T2)
            v = q_block(p_own, s_own)
            at(B, s_own - 2 * c, p_own)[...] = v.T
            tick(t, "Q", 1)
            a_wait(PP, PS, SP)
            v = q_block(i1, j1)
            stage[FIRST] = v.T
            b_copy(FIRST).start()
            tick(t, "Q", 2)
            a_wait(SS)
            v = q_block(i2, j2)
            stage[SECOND] = v.T
            b_copy(SECOND).start()
            tick(t, "Q", 3)
            q_block(s_own, s_own)
            tick(t, "Q", 4)
            for k in every:
                a_copy(k, *a_blocks[k]).wait_send()

            @pl.when(t > 0)
            def _():
                x_wait_send(cur)

        def y_step(t, cur, nxt):
            xt, xn = X.at[cur], X.at[nxt]
            for k, p in enumerate((p_own, s_own)):
                b_copy(k).wait_recv()

                @pl.loop(0, 4)
                def _(j):
                    cols = pl.ds(pl.multiple_of(j * blk, blk), blk)
                    y = dot(B[rows(p - 2 * c), :], xt[:, cols])
                    at(xn, p, j)[...] = blend(at(xt, p, j)[...], y)
                    x_copy(nxt, p, j, k).start()
                    tick(t, "PS"[k], j)
            for k in PAIR:
                b_copy(k).wait_send()

        @pl.loop(0, NS_STEPS - 1)
        def _(t):
            cur = lax.rem(t, 2)
            nxt = 1 - cur
            a_step(t, cur)
            q_step(t, cur)
            y_step(t, cur, nxt)

        last = NS_STEPS - 1
        cur = last % 2
        a_step(last, cur)
        a_wait(*every)
        for k in every:
            a_copy(k, *a_blocks[k]).wait_send()
        x_wait_send(cur)
        own = oa.shape[0]
        mine = pl.ds(pl.multiple_of(own * (base + 2 * c), 2 * own), 2 * own)
        for j in QUAD:
            cols = pl.ds(j * blk, blk)
            B[0:2 * own, cols] = poly(A[mine, cols], dot(A[mine, :], A[:, cols]))
        for j in QUAD:
            cols = pl.ds(j * blk, blk)
            obuf[0:2 * own, cols] = blend(X[cur, mine, cols], dot(B[0:2 * own, :], X[cur, :, cols]))

        def o_copy(k, target):
            return pltpu.make_async_remote_copy(obuf.at[pl.ds(own * k, own)], oa, osend.at[k], orecv.at[0],
                                                device_id=dev(target), device_id_type=MESH)

        @pl.when(c == 1)
        def _():
            o_copy(0, base + 2).start()
            o_copy(1, base + 3).start()
            o_copy(0, base + 2).wait_send()
            o_copy(1, base + 3).wait_send()

        @pl.when(c == 0)
        def _():
            o_copy(1, base + 1).start()
            oa[...] = obuf[0:own, :]
            o_copy(1, base + 1).wait_send()

    @pl.when(role >= 2)
    def _():
        for _, *calls in steps:
            run(calls)
        comm.ag_arrived(UP)
        comm.ag_arrived(DOWN)

        def load(full, place):
            own = full.shape[3]
            copies = [pltpu.make_async_copy(full.at[yy, xx, cc], place(pl.ds(((yy * side + xx) * 2 + cc) * own, own)),
                                            load_sem.at[(yy * side + xx) * 2 + cc])
                      for yy in range(side) for xx in range(side) for cc in PAIR]
            for cp in copies:
                cp.start()
            for cp in copies:
                cp.wait()

        @pl.when(role == 2)
        def _():
            load(xu, lambda rows_at: X.at[1, rows_at, pl.ds(0, half)])

            @pl.loop(0, 4)
            def _(i):
                for j in PAIR:
                    at(X.at[0], j, i)[...] = at(X.at[1], i, j)[...].T

        @pl.when(role == 3)
        def _():
            load(xd, lambda rows_at: X.at[0, rows_at])

        pairs = ((0, 0), (0, 1), (1, 1))

        def a_step(cur):
            for i, j in pairs:
                v = dot_nt(X[cur, i * blk:(i + 1) * blk, :], X[cur, j * blk:(j + 1) * blk, :]).astype(BF16)
                at(A, i, j)[...] = v
                if i != j:
                    at(A, j, i)[...] = v.T

        def q_step():
            for i, j in pairs:
                v = poly(at(A, i, j)[...], dot(A[i * blk:(i + 1) * blk, 0:half], A[0:half, j * blk:(j + 1) * blk]))
                at(B, i, j)[...] = v
                if i != j:
                    at(B, j, i)[...] = v.T

        @pl.loop(0, NS_STEPS - 1)
        def _(t):
            cur = lax.rem(t, 2)
            nxt = 1 - cur
            a_step(cur)

            q_step()

            @pl.loop(0, 4)
            def _(j):
                cols = pl.ds(pl.multiple_of(j * blk, blk), blk)
                for i in PAIR:
                    y = dot(B[i * blk:(i + 1) * blk, 0:half], X[cur, 0:half, cols])
                    at(X.at[nxt], i, j)[...] = blend(at(X.at[cur], i, j)[...], y)

        cur = (NS_STEPS - 1) % 2
        a_step(cur)

        @pl.when(role == 2)
        def _():
            own = ou.shape[0]
            cols = pl.ds(pl.multiple_of(own * base, 4 * own), 4 * own)
            q_step()
            for i in PAIR:
                o = blend(X[cur, i * blk:(i + 1) * blk, cols], dot(B[i * blk:(i + 1) * blk, 0:half], X[cur, 0:half, cols]))
                obuf[0:4 * own, i * blk:(i + 1) * blk] = o.T

            def o_copy(k):
                return pltpu.make_async_remote_copy(obuf.at[pl.ds(own * k, own), pl.ds(0, half)], ou, osend.at[k], orecv.at[1],
                                                    device_id=dev(base + k), device_id_type=MESH)
            for k in (0, 1, 3):
                o_copy(k).start()
            ou[...] = obuf[2 * own:3 * own, 0:half]
            for k in (0, 1, 3):
                o_copy(k).wait_send()

        @pl.when(role == 3)
        def _():
            own = od.shape[0]
            mine = pl.ds(pl.multiple_of(own * base, 4 * own), 4 * own)
            for j in PAIR:
                cols = pl.ds(j * blk, blk)
                B[0:4 * own, cols] = poly(A[mine, cols], dot(A[mine, 0:half], A[0:half, cols]))
            for j in QUAD:
                cols = pl.ds(j * blk, blk)
                obuf[0:4 * own, cols] = blend(X[cur, mine, cols], dot(B[0:4 * own, 0:half], X[cur, 0:half, cols]))

            def o_copy(k):
                return pltpu.make_async_remote_copy(obuf.at[pl.ds(own * k, own)], od, osend.at[k], orecv.at[2],
                                                    device_id=dev(base + k), device_id_type=MESH)
            for k in (0, 1, 2):
                o_copy(k).start()
            od[...] = obuf[3 * own:4 * own, :]
            for k in (0, 1, 2):
                o_copy(k).wait_send()

    def arrived(o, k):
        pltpu.make_async_remote_copy(o, o, osend.at[k], orecv.at[k], device_id=dev(base), device_id_type=MESH).wait_recv()

    @pl.when(role != 3)
    def _():
        arrived(od, 2)
    od_out[...] = od[...]

    @pl.when(role != 2)
    def _():
        arrived(ou, 1)
    ou_out[...] = ou[...]

    @pl.when(role != 0)
    def _():
        arrived(oa, 0)
    oa_out[...] = oa[...]
    comm.finish()
    comm.ag_finish(UP)
    comm.ag_finish(DOWN)


def orthogonalize(side, ax, xa, xu, grad_down, mom_down):
    n = xa.shape[1]
    blk = n // 4
    group = 2 * side * side
    dma = pltpu.SemaphoreType.DMA
    vmem = pl.BlockSpec(memory_space=pltpu.VMEM)
    hbm = pl.BlockSpec(memory_space=pl.ANY)
    own_a, own_u, own_d = (n // group, n), xu.shape, mom_down.shape
    scratch = [
        pltpu.VMEM((2, n, n), BF16),
        pltpu.VMEM((n, n), BF16),
        pltpu.VMEM((n // 2, n), BF16),
        pltpu.VMEM((2, blk, blk), BF16),
        pltpu.VMEM((4 * max(own_a[0], own_u[0]), n), BF16),
        pltpu.VMEM(own_a, BF16),
        pltpu.VMEM(own_u, BF16),
        pltpu.VMEM(own_d, BF16),
    ]
    scratch += scratch_for(side, [own_d]) + [pltpu.VMEM(own_d, BF16), pltpu.VMEM((3, 3, side, 8, 128), F32)]
    scratch += [dma((group,)), dma((8,)), dma((8,)), dma((2,)), dma((2,)), dma((2, 4)), dma((2, 4)), dma((4,)), dma((3,))]
    scratch += [dma((20,)), dma((90,)), dma((90,))]
    oa, ou, od, nd, _, _ = pl.pallas_call(
        functools.partial(ns_kernel, n, side, group, ax),
        name="newton_schulz",
        out_shape=[jax.ShapeDtypeStruct(s, BF16) for s in (own_a, own_u, own_d)]
        + [jax.ShapeDtypeStruct(own_d, F32)]
        + [jax.ShapeDtypeStruct((side, side, 2) + s, BF16) for s in (own_u, own_d)],
        in_specs=[hbm, vmem, hbm, vmem],
        out_specs=[vmem] * 4 + [hbm] * 2,
        scratch_shapes=scratch,
        compiler_params=pltpu.CompilerParams(collective_id=1, has_side_effects=True, vmem_limit_bytes=VMEM_LIMIT),
    )(xa, xu, grad_down.reshape(side, side, 2, *own_d), mom_down)
    return oa, ou, od, nd


def update_kernel(scales, *refs):
    for k, scale in enumerate(scales):
        o, new, w = refs[3 * k:3 * k + 3]
        new_out, w_out, b_out = refs[9 + 3 * k:12 + 3 * k]
        new_out[...] = new[...]
        old = w[...]
        updated = old - LEARN_RATE * (scale * o[...].astype(F32) + WEIGHT_DECAY * old)
        w_out[...] = updated
        b_out[...] = updated.astype(BF16)


def update(group, orthos, moms, masters):
    args, outs, scales = [], [], []
    for o, new, w in zip(orthos, moms, masters):
        args += [o, new, w]
        outs += [jax.ShapeDtypeStruct(w.shape, F32)] * 2 + [jax.ShapeDtypeStruct(w.shape, BF16)]
        scales.append(0.2 * math.sqrt(max(group * w.shape[0], w.shape[1])))
    vmem = pl.BlockSpec(memory_space=pltpu.VMEM)
    return pl.pallas_call(
        functools.partial(update_kernel, scales), name="update", out_shape=outs,
        in_specs=[vmem] * 9, out_specs=[vmem] * 9,
    )(*args)


def solution(mesh):
    ax = mesh.axis_names[1]
    group = mesh.shape[ax]
    side = math.isqrt(group // 2)
    grad_spec = P(tuple(mesh.axis_names), None, None, None)
    row_spec = P(mesh.axis_names[0], ax, None)

    def step_local(*arrays):
        grads = [arrays[3 * k][0, 0] for k in range(3)]
        moms = [arrays[3 * k + 1][0] for k in range(3)]
        masters = [arrays[3 * k + 2][0] for k in range(3)]
        na, nu, xu, xa = reduce_and_gather(side, ax, grads[:2], moms[:2])
        oa, ou, od, nd = orthogonalize(side, ax, xa, xu, grads[2], moms[2])
        return tuple(r[None] for r in update(group, (oa, ou, od), (na, nu, nd), masters))

    return jax.shard_map(step_local, mesh=mesh, in_specs=(grad_spec, row_spec, row_spec) * 3,
                         out_specs=(row_spec,) * 9, check_vma=False)
```

```python
import functools
import math

import jax
import jax.numpy as jnp
from jax import lax
from jax.experimental import pallas as pl
from jax.experimental.pallas import tpu as pltpu
from jax.sharding import PartitionSpec as P

MOMENTUM = 0.95
LEARN_RATE = 0.25
WEIGHT_DECAY = 0.2
EPSILON = 1e-7
COEF_A = 3.4445
COEF_B = -4.7750
COEF_C = 2.0315
NS_STEPS = 5
F32 = jnp.float32
BF16 = jnp.bfloat16
MESH = pl.DeviceIdType.MESH
VMEM_LIMIT = 66_000_000
ATTN, UP, DOWN = MATRICES = range(3)
FIRST, SECOND = PAIR = range(2)
ALL = slice(None)
QUAD = range(4)


class Comm:
    def __init__(self, side, group, ax, mats, slots, local_sem, send_sem, recv_sem):
        self.side, self.group, self.ax, self.mats, self.slots = side, group, ax, mats, slots
        self.local_sem, self.send_sem, self.recv_sem = local_sem, send_sem, recv_sem
        me = lax.axis_index(ax)
        self.role = lax.rem(me, 4)
        self.c = lax.rem(me, 2)
        self.x = lax.rem(me // 2, side)
        self.y = me // (2 * side)
        self.peer = self.dev(self.y, self.x, 1 - self.c)
        self.pos = ((self.x, self.y), (self.y, self.x))
        self.keys, self.local_keys, self.sent, self.peer_only = {}, {}, {}, {}

    def dev(self, yy, xx, cc):
        return {self.ax: (lax.rem(yy, self.side) * self.side + lax.rem(xx, self.side)) * 2 + cc}

    def greet(self):
        barrier = pltpu.get_barrier_semaphore()
        pl.semaphore_signal(barrier, inc=1, device_id=self.peer, device_id_type=MESH)
        for k in range(1, self.side):
            pl.semaphore_signal(barrier, inc=1, device_id=self.dev(self.y + k, self.x, self.c), device_id_type=MESH)
            pl.semaphore_signal(barrier, inc=1, device_id=self.dev(self.y, self.x + k, self.c), device_id_type=MESH)
        return 2 * self.side - 1

    def to(self, along_x, step):
        step = step % self.side
        return self.dev(self.y, self.x + step, self.c) if along_x else self.dev(self.y + step, self.x, self.c)

    def remote(self, key, src, dst, target):
        k = self.keys.setdefault(key, len(self.keys))
        return pltpu.make_async_remote_copy(src, dst, self.send_sem.at[k], self.recv_sem.at[k],
                                            device_id=target, device_id_type=MESH)

    def local(self, key, src, dst):
        k = self.local_keys.setdefault(key, len(self.local_keys))
        return pltpu.make_async_copy(src, dst, self.local_sem.at[k])

    def start(self, make, *args):
        make(*args).start()
        self.sent[(make.__name__,) + args] = (make, args)

    def finish(self):
        for make, args in self.sent.values():
            make(*args).wait_send()

    def shift(self, p, k):
        return lax.rem(p + k, self.side)

    def quarter(self, m, f, h):
        q = self.mats[m]["own"].shape[-1] // 4
        return pl.ds((2 * f + h) * q, q)

    def half(self, m, f):
        q = self.mats[m]["own"].shape[-1] // 2
        return pl.ds(f * q, q)

    @staticmethod
    def lane1(f, k):
        return (ALL, k) if f == 0 else (k, ALL)

    def lane2(self, f, k):
        return (k, self.x) if f == 0 else (self.y, k)

    @staticmethod
    def one(f, k, i):
        return (i, k) if f == 0 else (k, i)

    def pair_remote(self, m, f, k):
        idx = self.lane1(f, self.shift(self.pos[f][0], k))
        cols = self.half(m, f)
        mat = self.mats[m]
        return self.remote(("pair", m, f, k), mat["grad"].at[idx + (1 - self.c, ALL, cols)],
                           mat["peer"].at[idx + (ALL, cols)], self.peer)

    def pair_local(self, m, f, k):
        idx = self.lane1(f, self.shift(self.pos[f][0], k))
        cols = self.half(m, f)
        mat = self.mats[m]
        return self.local(("pair", m, f, k), mat["grad"].at[idx + (self.c, ALL, cols)],
                          mat["sum"].at[idx + (ALL, cols)])

    def pair_start(self, m):
        for k in (2, 1, self.side - 1, 0):
            for f in PAIR:
                self.start(self.pair_remote, m, f, k)
                self.pair_local(m, f, k).start()

    def pair_sum(self, m, f, k):
        self.pair_remote(m, f, k).wait_recv()
        self.pair_local(m, f, k).wait()
        kk = self.shift(self.pos[f][0], k)
        cols = self.half(m, f)
        total, other = self.mats[m]["sum"], self.mats[m]["peer"]

        @pl.loop(0, self.side)
        def _(i):
            idx = self.one(f, kk, i) + (ALL, cols)
            total[idx] = total[idx] + other[idx]

    def ring(self, m, f, phase, j):
        k, h, step = ((2, 1, 1), (2, 0, -1), (1, 0, 1), (-1, 1, -1), (1, 1, 1), (-1, 0, -1))[j]
        kk = self.shift(self.pos[f][phase], k % self.side)
        idx = (self.lane1, self.lane2)[phase](f, kk) + (ALL, self.quarter(m, f, h))
        mat = self.mats[m]
        return self.remote(("ring", m, f, phase, j), mat["sum"].at[idx], mat[("ring1", "ring2")[phase]].at[f, j],
                           self.to((f == 0) == (phase == 0), step))

    def ring_add(self, m, f, phase, j, k, h):
        self.ring(m, f, phase, j).wait_recv()
        kk = self.shift(self.pos[f][phase], k % self.side)
        cols = self.quarter(m, f, h)
        mat = self.mats[m]
        total = mat["sum"]
        if phase == 0:
            @pl.loop(0, self.side)
            def _(i):
                idx = self.one(f, kk, i) + (ALL, cols)
                total[idx] = total[idx] + mat["ring1"][f, j, i]
        else:
            idx = self.lane2(f, kk) + (ALL, cols)
            total[idx] = total[idx] + mat["ring2"][f, j]

    def rs_far(self, m):
        for f in PAIR:
            self.pair_sum(m, f, 2)
            self.start(self.ring, m, f, 0, 0)
            self.start(self.ring, m, f, 0, 1)

    def rs_near(self, m):
        for f in PAIR:
            self.pair_sum(m, f, 1)
            self.start(self.ring, m, f, 0, 2)
            self.pair_sum(m, f, self.side - 1)
            self.start(self.ring, m, f, 0, 3)

    def rs_own(self, m):
        for f in PAIR:
            self.pair_sum(m, f, 0)

    def pass_on(self, m, phase):
        for f in PAIR:
            self.ring_add(m, f, phase, 0, 1, 1)
            self.start(self.ring, m, f, phase, 4)
            self.ring_add(m, f, phase, 1, -1, 0)
            self.start(self.ring, m, f, phase, 5)

    def settle(self, m, phase):
        for f in PAIR:
            for j, h in ((2, 0), (3, 1), (4, 1), (5, 0)):
                self.ring_add(m, f, phase, j, 0, h)
            if phase == 0:
                for j in range(4):
                    self.start(self.ring, m, f, 1, j)

    def norm_pair(self, m):
        ref = self.slots.at[m, 0, self.c]
        return self.remote(("norm", m), ref, ref, self.peer)

    def norm_line(self, m, level, k):
        ref = self.slots.at[m, level, self.x if level == 1 else self.y]
        return self.remote(("norm", m, level, k), ref, ref, self.to(level == 1, k))

    def momentum(self, m):
        mat = self.mats[m]
        mat["new"][...] = MOMENTUM * mat["mom"][...] + mat["sum"][self.y, self.x] / self.group

    def squares(self, m):
        mat = self.mats[m]
        rows, cols = mat["new"].shape
        acc = jnp.zeros((8, 128), F32)
        for i in range(0, rows, 8):
            for j in range(0, cols, 128):
                part = mat["new"][i:i + 8, j:j + 128]
                acc = acc + part * part
        self.slots[m, 0, self.c] = acc
        self.start(self.norm_pair, m)

    def norm_x(self, m):
        self.norm_pair(m).wait_recv()
        self.slots[m, 1, self.x] = self.slots[m, 0, 0] + self.slots[m, 0, 1]
        for k in range(1, self.side):
            self.start(self.norm_line, m, 1, k)

    def level_sum(self, m, level):
        for k in range(1, self.side):
            self.norm_line(m, level, k).wait_recv()
        acc = self.slots[m, level, 0]
        for k in range(1, self.side):
            acc = acc + self.slots[m, level, k]
        return acc

    def norm_y(self, m):
        self.slots[m, 2, self.y] = self.level_sum(m, 1)
        for k in range(1, self.side):
            self.start(self.norm_line, m, 2, k)

    def normalize(self, m):
        mat = self.mats[m]
        norm = jnp.sqrt(jnp.sum(self.level_sum(m, 2), axis=(0, 1), keepdims=True))
        mat["own"][...] = (mat["new"][...] / (norm + EPSILON)).astype(BF16)

    def along(self, f, phase):
        return (f == 0) != (phase == 0)

    def gpos(self, f, phase):
        return self.x if self.along(f, phase) else self.y

    def spot(self, m, f, phase, k, cols):
        if phase == 0:
            idx = (k, self.x) if f == 0 else (self.y, k)
        else:
            idx = self.lane1(f, k)
        return self.mats[m]["full"].at[idx + (self.c, ALL, cols)]

    def ag_own(self, m):
        return self.local(("own", m), self.mats[m]["own"], self.mats[m]["full"].at[self.y, self.x, self.c])

    def ag_send(self, m, f, phase, j):
        dst = self.spot(m, f, phase, self.gpos(f, phase), self.half(m, f))
        src = self.mats[m]["own"].at[:, self.half(m, f)] if phase == 0 else dst
        return self.remote(("send", m, f, phase, j), src, dst, self.to(self.along(f, phase), (1, -1)[j]))

    def ag_relay(self, m, f, phase, j):
        ref = self.spot(m, f, phase, self.shift(self.gpos(f, phase), (self.side - 1, 1)[j]), self.quarter(m, f, (1, 0)[j]))
        return self.remote(("relay", m, f, phase, j), ref, ref, self.to(self.along(f, phase), (1, -1)[j]))

    def ag_peer(self, m, f, k):
        ref = self.spot(m, f, 1, self.shift(self.gpos(f, 1), k), self.half(m, f))
        return self.remote(("peer", m, f, k), ref, ref, self.peer)

    def to_peer(self, m, f, k):
        self.peer_only[m, f, k] = True

        @pl.when(self.sends(m))
        def _():
            self.ag_peer(m, f, k).start()

    def sends(self, m):
        return self.role < 2 if m == 0 else self.role == 4 - m

    def needs(self, m):
        return self.role < 2 if m == 0 else self.role == 1 + m

    def ag_start(self, m):
        self.ag_own(m).start()
        for f in PAIR:
            for j in PAIR:
                self.start(self.ag_send, m, f, 0, j)

    def ag_forward(self, m, phase):
        for f in PAIR:
            for j in PAIR:
                self.ag_send(m, f, phase, j).wait_recv()
                self.start(self.ag_relay, m, f, phase, j)
                if phase == 1:
                    self.to_peer(m, f, (self.side - 1, 1)[j])

    def ag_turn(self, m):
        self.ag_own(m).wait()
        for f in PAIR:
            for j in PAIR:
                self.ag_relay(m, f, 0, j).wait_recv()
            for j in PAIR:
                self.start(self.ag_send, m, f, 1, j)
            self.to_peer(m, f, 0)

    def ag_end(self, m):
        for f in PAIR:
            for j in PAIR:
                self.ag_relay(m, f, 1, j).wait_recv()
            self.to_peer(m, f, 2)

    def ag_arrived(self, m):
        @pl.when(self.needs(m))
        def _():
            for f in PAIR:
                for k in range(self.side):
                    self.ag_peer(m, f, k).wait_recv()

    def ag_finish(self, m):
        @pl.when(self.sends(m))
        def _():
            for f in PAIR:
                for k in range(self.side):
                    self.ag_peer(m, f, k).wait_send()


def reduce_kernel(side, group, ax, ga, gu, gd, ma, mu, md, na, nu, nd, xa,
                  sa, su, sd, pa, pu, pd, ra1, ru1, rd1, ra2, ru2, rd2, xra, xru, xrd, slots, local_sem, send_sem, recv_sem):
    mats = {ATTN: dict(grad=ga, mom=ma, new=na, full=xa, sum=sa, peer=pa, ring1=ra1, ring2=ra2, own=xra),
            UP: dict(grad=gu, mom=mu, new=nu, sum=su, peer=pu, ring1=ru1, ring2=ru2, own=xru),
            DOWN: dict(grad=gd, mom=md, new=nd, sum=sd, peer=pd, ring1=rd1, ring2=rd2, own=xrd)}
    comm = Comm(side, group, ax, mats, slots, local_sem, send_sem, recv_sem)
    pl.semaphore_wait(pltpu.get_barrier_semaphore(), comm.greet())
    comm.pair_start(ATTN)
    comm.pair_start(UP)
    comm.pair_start(DOWN)
    comm.rs_far(ATTN)
    comm.rs_near(ATTN)
    comm.rs_own(ATTN)
    comm.pass_on(ATTN, FIRST)
    comm.rs_far(UP)
    comm.settle(ATTN, FIRST)
    comm.rs_near(UP)
    comm.pass_on(ATTN, SECOND)
    comm.rs_own(UP)
    comm.pass_on(UP, FIRST)
    comm.settle(ATTN, SECOND)
    comm.momentum(ATTN)
    comm.squares(ATTN)
    comm.rs_far(DOWN)
    comm.norm_x(ATTN)
    comm.rs_near(DOWN)
    comm.norm_y(ATTN)
    comm.normalize(ATTN)
    comm.ag_start(ATTN)
    comm.settle(UP, FIRST)
    comm.rs_own(DOWN)
    comm.pass_on(DOWN, FIRST)
    comm.ag_forward(ATTN, FIRST)
    comm.pass_on(UP, SECOND)
    comm.ag_turn(ATTN)
    comm.settle(DOWN, FIRST)
    comm.settle(UP, SECOND)
    comm.momentum(UP)
    comm.pass_on(DOWN, SECOND)
    comm.ag_forward(ATTN, SECOND)
    comm.settle(DOWN, SECOND)
    comm.momentum(DOWN)
    comm.ag_end(ATTN)
    comm.ag_arrived(ATTN)
    comm.finish()
    comm.ag_finish(ATTN)


def scratch_for(side, shapes):
    scratch = [pltpu.VMEM((side, side) + s, F32) for s in shapes] * 2
    scratch += [pltpu.VMEM((2, 6, side, s[0], s[1] // 4), F32) for s in shapes]
    scratch += [pltpu.VMEM((2, 6, s[0], s[1] // 4), F32) for s in shapes]
    return scratch


def reduce_and_gather(side, ax, grads, moms):
    dma = pltpu.SemaphoreType.DMA
    vmem = pl.BlockSpec(memory_space=pltpu.VMEM)
    hbm = pl.BlockSpec(memory_space=pl.ANY)
    group = 2 * side * side
    shapes = [m.shape for m in moms]
    views = [g.reshape(side, side, 2, *s) for g, s in zip(grads, shapes)]
    scratch = scratch_for(side, shapes) + [pltpu.VMEM(each, BF16) for each in shapes]
    scratch += [pltpu.VMEM((2, 3, side, 8, 128), F32), dma((30,)), dma((130,)), dma((130,))]
    na, nu, nd, xa = pl.pallas_call(
        functools.partial(reduce_kernel, side, group, ax),
        name="reduce_gather",
        out_shape=[jax.ShapeDtypeStruct(s, F32) for s in shapes]
        + [jax.ShapeDtypeStruct((side, side, 2) + shapes[0], BF16)],
        in_specs=[hbm] * 3 + [vmem] * 3,
        out_specs=[vmem] * 3 + [hbm],
        scratch_shapes=scratch,
        compiler_params=pltpu.CompilerParams(collective_id=0, has_side_effects=True, vmem_limit_bytes=VMEM_LIMIT),
    )(*views, *moms)
    return na, nu, nd, xa.reshape(group * shapes[0][0], shapes[0][1])


def ns_kernel(n, side, group, ax, xa, nu, nd, oa_out, ou_out, od_out, xu, xd,
              X, A, B, stage, obuf, oa, ou, od, xru, xrd, slots,
              load_sem, asend, arecv, bsend, brecv, xsend, xrecv, osend, orecv, local_sem, send_sem, recv_sem):
    me = lax.axis_index(ax)
    role = lax.rem(me, 4)
    base = me - role
    mats = {UP: dict(new=nu, full=xu, own=xru),
            DOWN: dict(new=nd, full=xd, own=xrd)}
    comm = Comm(side, group, ax, mats, slots, local_sem, send_sem, recv_sem)
    blk = n // 4
    half = n // 2

    def dev(k):
        return {ax: k}

    barrier = pltpu.get_barrier_semaphore()
    greeted = comm.greet()
    for step in range(1, 4):
        pl.semaphore_signal(barrier, inc=1, device_id=dev(base + lax.rem(role + step, 4)), device_id_type=MESH)
    pl.semaphore_wait(barrier, greeted + 3)
    comm.squares(UP)
    comm.squares(DOWN)
    steps = (
        ("0L0", (comm.norm_x, UP), (comm.norm_x, DOWN)),
        ("0A1", (comm.norm_y, UP), (comm.norm_y, DOWN)),
        ("0Q0", (comm.normalize, UP), (comm.ag_start, UP), (comm.normalize, DOWN), (comm.ag_start, DOWN)),
        ("0Y0", (comm.ag_forward, UP, FIRST), (comm.ag_forward, DOWN, FIRST)),
        ("0Y3", (comm.ag_turn, UP), (comm.ag_turn, DOWN)),
        ("1Q2", (comm.ag_forward, UP, SECOND)),
        ("1Y0", (comm.ag_forward, DOWN, SECOND)),
        ("1Y1", (comm.ag_end, UP)),
        ("1Y3", (comm.ag_end, DOWN)),
    )

    def run(calls):
        for call, *what in calls:
            call(*what)

    def tick(t, part, i):
        if isinstance(t, int):
            return
        for (when, where, block), *calls in steps:
            if where == part:
                go = jnp.logical_and(t == int(when), i == int(block))
                pl.when(go)(functools.partial(run, calls))

    def at(ref, i, j):
        return ref.at[pl.ds(pl.multiple_of(i * blk, blk), blk), pl.ds(pl.multiple_of(j * blk, blk), blk)]

    def rows(i, size=blk):
        return pl.ds(pl.multiple_of(i * size, size), size)

    def poly(a, q):
        return (COEF_B * a.astype(F32) + COEF_C * q.astype(BF16).astype(F32)).astype(BF16)

    def blend(x, y):
        return (COEF_A * x.astype(F32) + y.astype(BF16).astype(F32)).astype(BF16)

    def dot_nt(a, b):
        return lax.dot_general(a, b, (((1,), (1,)), ((), ())), preferred_element_type=F32)

    def dot(a, b):
        return jnp.dot(a, b, preferred_element_type=F32)

    @pl.when(role < 2)
    def _():
        c = role
        peer = dev(base + 1 - c)
        p_own, s_own = 3 * c, 1 + c
        p_peer, s_peer = 3 - 3 * c, 2 - c
        i1, j1 = 1 + 2 * c, 3 - 3 * c
        i2, j2 = 2 * c, 2 - c

        loads = [pltpu.make_async_copy(xa.at[rows(p)], X.at[0, rows(p)], load_sem.at[k])
                 for k, p in enumerate((p_own, s_own, p_peer, s_peer))]
        for cp in loads:
            cp.start()
        for cp in loads[:2]:
            cp.wait()

        def a_copy(k, i, j):
            return pltpu.make_async_remote_copy(at(A, i, j), at(A, i, j), asend.at[k], arecv.at[k],
                                                device_id=peer, device_id_type=MESH)

        a_blocks = ((p_own, p_own), (p_own, s_own), (s_own, p_own), (i1, j1), (j1, i1), (i2, j2), (j2, i2), (s_own, s_own))
        PP, PS, SP, C1, T1, C2, T2, SS = every = range(len(a_blocks))

        def a_send(k):
            a_copy(k, *a_blocks[k]).start()

        def a_wait(*ks):
            for k in ks:
                a_copy(k, *a_blocks[k]).wait_recv()

        mine = pl.ds(pl.multiple_of(half * c, half), half)

        def x_copy(nxt, j):
            ref = X.at[nxt, mine, pl.ds(pl.multiple_of(j * blk, blk), blk)]
            return pltpu.make_async_remote_copy(ref, ref, xsend.at[j], xrecv.at[j], device_id=peer, device_id_type=MESH)

        def b_copy(k):
            i, j = ((i1, j1), (i2, j2))[k]
            return pltpu.make_async_remote_copy(stage.at[k], at(B, j - 2 * (1 - c), i), bsend.at[k], brecv.at[k],
                                                device_id=peer, device_id_type=MESH)

        def gram(xt, i, j, mirror):
            v = dot_nt(xt[rows(i), :], xt[rows(j), :]).astype(BF16)
            at(A, i, j)[...] = v
            if mirror:
                at(A, j, i)[...] = v.T

        def col(j):
            return pl.ds(pl.multiple_of(j * blk, blk), blk)

        def a_step(t, cur):
            xt = X.at[cur]
            A[mine, col(p_own)] = dot_nt(xt[mine, :], xt[rows(p_own), :]).astype(BF16)
            at(A, p_own, s_own)[...] = at(A, s_own, p_own)[...].T

            @pl.when(t > 0)
            def _():
                for j in QUAD:
                    x_copy(cur, j).wait_recv()
            a_send(PP)
            a_send(SP)
            a_send(PS)
            tick(t, "A", 0)

            @pl.when(t == 0)
            def _():
                for cp in loads[2:]:
                    cp.wait()
            gram(xt, i1, j1, True)
            a_send(C1)
            a_send(T1)
            tick(t, "A", 1)
            gram(xt, i2, j2, True)
            a_send(C2)
            a_send(T2)
            tick(t, "A", 2)
            gram(xt, s_own, s_own, False)
            a_send(SS)
            tick(t, "A", 3)

        def sent(t, cur):
            for k in every:
                a_copy(k, *a_blocks[k]).wait_send()

            @pl.when(t > 0)
            def _():
                for j in QUAD:
                    x_copy(cur, j).wait_send()

        def q_block(i, j):
            v = poly(at(A, i, j)[...], dot(A[rows(i), :], A[:, col(j)]))
            at(B, i - 2 * c, j)[...] = v
            return v

        def q_step(t, cur):
            a_wait(C1, T1)
            q_block(p_own, p_own)
            tick(t, "Q", 0)
            a_wait(C2, T2, PP, PS, SP)
            stage[FIRST] = q_block(i1, j1).T
            b_copy(FIRST).start()
            tick(t, "Q", 1)
            a_wait(SS)
            stage[SECOND] = q_block(i2, j2).T
            b_copy(SECOND).start()
            tick(t, "Q", 2)
            B[:, col(s_own)] = poly(A[mine, col(s_own)], dot(A[mine, :], A[:, col(s_own)]))
            at(B, s_own - 2 * c, p_own)[...] = at(B, p_own - 2 * c, s_own)[...].T
            tick(t, "Q", 3)
            sent(t, cur)

        def y_step(t, cur, nxt):
            xt, xn = X.at[cur], X.at[nxt]
            for k in PAIR:
                b_copy(k).wait_recv()

            @pl.loop(0, 4)
            def _(j):
                xn[mine, col(j)] = blend(xt[mine, col(j)], dot(B[...], xt[:, col(j)]))
                x_copy(nxt, j).start()
                tick(t, "Y", j)
            for k in PAIR:
                b_copy(k).wait_send()

        for where, *calls in steps:
            if "L" in where:
                run(calls)
        last = NS_STEPS - 1

        @pl.loop(0, NS_STEPS)
        def _(t):
            cur = lax.rem(t, 2)
            a_step(t, cur)

            @pl.when(t < last)
            def _():
                q_step(t, cur)
                y_step(t, cur, 1 - cur)

        cur = last % 2
        a_wait(*every)
        sent(last, cur)
        own = oa.shape[0]
        ours = pl.ds(pl.multiple_of(own * (base + 2 * c), 2 * own), 2 * own)
        for j in QUAD:
            cols = pl.ds(j * blk, blk)
            B[0:2 * own, cols] = poly(A[ours, cols], dot(A[ours, :], A[:, cols]))

        def o_copy(k, target, j):
            cols = pl.ds(j * blk, blk)
            return pltpu.make_async_remote_copy(obuf.at[pl.ds(own * k, own), cols], oa.at[:, cols], osend.at[4 * k + j],
                                                orecv.at[j], device_id=dev(target), device_id_type=MESH)

        for j in QUAD:
            cols = pl.ds(j * blk, blk)
            obuf[0:2 * own, cols] = blend(X[cur, ours, cols], dot(B[0:2 * own, :], X[cur, :, cols]))

            @pl.when(c == 1)
            def _():
                o_copy(FIRST, base + 2, j).start()
                o_copy(SECOND, base + 3, j).start()

            @pl.when(c == 0)
            def _():
                o_copy(SECOND, base + 1, j).start()

        @pl.when(c == 1)
        def _():
            for j in QUAD:
                o_copy(FIRST, base + 2, j).wait_send()
                o_copy(SECOND, base + 3, j).wait_send()

        @pl.when(c == 0)
        def _():
            oa[...] = obuf[0:own, :]
            for j in QUAD:
                o_copy(SECOND, base + 1, j).wait_send()

    @pl.when(role >= 2)
    def _():
        for _, *calls in steps:
            run(calls)
        comm.ag_arrived(UP)
        comm.ag_arrived(DOWN)

        def load(full, place):
            own = full.shape[3]
            copies = [pltpu.make_async_copy(full.at[yy, xx, cc], place(pl.ds(((yy * side + xx) * 2 + cc) * own, own)),
                                            load_sem.at[(yy * side + xx) * 2 + cc])
                      for yy in range(side) for xx in range(side) for cc in PAIR]
            for cp in copies:
                cp.start()
            for cp in copies:
                cp.wait()

        @pl.when(role == 2)
        def _():
            load(xu, lambda rows_at: X.at[1, rows_at, pl.ds(0, half)])

            @pl.loop(0, 4)
            def _(i):
                for j in PAIR:
                    at(X.at[0], j, i)[...] = at(X.at[1], i, j)[...].T

        @pl.when(role == 3)
        def _():
            load(xd, lambda rows_at: X.at[0, rows_at])

        def a_step(cur):
            A[0:half, 0:blk] = dot_nt(X[cur, 0:half, :], X[cur, 0:blk, :]).astype(BF16)
            A[0:blk, blk:half] = A[blk:half, 0:blk].T
            A[blk:half, blk:half] = dot_nt(X[cur, blk:half, :], X[cur, blk:half, :]).astype(BF16)

        def q_step():
            B[0:half, 0:blk] = poly(A[0:half, 0:blk], dot(A[0:half, 0:half], A[0:half, 0:blk]))
            B[0:blk, blk:half] = B[blk:half, 0:blk].T
            B[blk:half, blk:half] = poly(A[blk:half, blk:half], dot(A[blk:half, 0:half], A[0:half, blk:half]))

        @pl.loop(0, NS_STEPS)
        def _(t):
            cur = lax.rem(t, 2)
            a_step(cur)

            @pl.when(jnp.logical_or(t < NS_STEPS - 1, role == 2))
            def _():
                q_step()

            @pl.when(t < NS_STEPS - 1)
            def _():
                @pl.loop(0, 4)
                def _(j):
                    cols = pl.ds(pl.multiple_of(j * blk, blk), blk)
                    y = dot(B[0:half, 0:half], X[cur, 0:half, cols])
                    X[1 - cur, 0:half, cols] = blend(X[cur, 0:half, cols], y)

        cur = (NS_STEPS - 1) % 2

        @pl.when(role == 2)
        def _():
            own = ou.shape[0]
            cols = pl.ds(pl.multiple_of(own * base, 4 * own), 4 * own)
            for i in PAIR:
                o = blend(X[cur, i * blk:(i + 1) * blk, cols], dot(B[i * blk:(i + 1) * blk, 0:half], X[cur, 0:half, cols]))
                obuf[0:4 * own, i * blk:(i + 1) * blk] = o.T

            def o_copy(k):
                return pltpu.make_async_remote_copy(obuf.at[pl.ds(own * k, own), pl.ds(0, half)], ou, osend.at[k], orecv.at[4],
                                                    device_id=dev(base + k), device_id_type=MESH)
            for k in (0, 1, 3):
                o_copy(k).start()
            ou[...] = obuf[2 * own:3 * own, 0:half]
            for k in (0, 1, 3):
                o_copy(k).wait_send()

        @pl.when(role == 3)
        def _():
            own = od.shape[0]
            mine = pl.ds(pl.multiple_of(own * base, 4 * own), 4 * own)
            for j in PAIR:
                cols = pl.ds(j * blk, blk)
                B[0:4 * own, cols] = poly(A[mine, cols], dot(A[mine, 0:half], A[0:half, cols]))
            for j in QUAD:
                cols = pl.ds(j * blk, blk)
                obuf[0:4 * own, cols] = blend(X[cur, mine, cols], dot(B[0:4 * own, 0:half], X[cur, 0:half, cols]))

            def o_copy(k):
                return pltpu.make_async_remote_copy(obuf.at[pl.ds(own * k, own)], od, osend.at[k], orecv.at[5],
                                                    device_id=dev(base + k), device_id_type=MESH)
            for k in (0, 1, 2):
                o_copy(k).start()
            od[...] = obuf[3 * own:4 * own, :]
            for k in (0, 1, 2):
                o_copy(k).wait_send()

    def arrived(o, k):
        pltpu.make_async_remote_copy(o, o, osend.at[k], orecv.at[k], device_id=dev(base), device_id_type=MESH).wait_recv()

    @pl.when(role != 3)
    def _():
        arrived(od, 5)
    od_out[...] = od[...]

    @pl.when(role != 2)
    def _():
        arrived(ou, 4)
    ou_out[...] = ou[...]

    @pl.when(role != 0)
    def _():
        for j in QUAD:
            arrived(oa.at[:, pl.ds(j * blk, blk)], j)
    oa_out[...] = oa[...]
    comm.finish()
    comm.ag_finish(UP)
    comm.ag_finish(DOWN)


def orthogonalize(side, ax, xa, mom_up, mom_down):
    n = xa.shape[1]
    blk = n // 4
    group = 2 * side * side
    dma = pltpu.SemaphoreType.DMA
    vmem = pl.BlockSpec(memory_space=pltpu.VMEM)
    hbm = pl.BlockSpec(memory_space=pl.ANY)
    own_a, own_u, own_d = (n // group, n), mom_up.shape, mom_down.shape
    scratch = [
        pltpu.VMEM((2, n, n), BF16),
        pltpu.VMEM((n, n), BF16),
        pltpu.VMEM((n // 2, n), BF16),
        pltpu.VMEM((2, blk, blk), BF16),
        pltpu.VMEM((4 * max(own_a[0], own_u[0]), n), BF16),
        pltpu.VMEM(own_a, BF16),
        pltpu.VMEM(own_u, BF16),
        pltpu.VMEM(own_d, BF16),
    ]
    scratch += [pltpu.VMEM(own_u, BF16), pltpu.VMEM(own_d, BF16), pltpu.VMEM((3, 3, side, 8, 128), F32)]
    scratch += [dma((group,)), dma((8,)), dma((8,)), dma((2,)), dma((2,)), dma((4,)), dma((4,)), dma((8,)), dma((6,))]
    scratch += [dma((20,)), dma((110,)), dma((110,))]
    oa, ou, od, _, _ = pl.pallas_call(
        functools.partial(ns_kernel, n, side, group, ax),
        name="newton_schulz",
        out_shape=[jax.ShapeDtypeStruct(s, BF16) for s in (own_a, own_u, own_d)]
        + [jax.ShapeDtypeStruct((side, side, 2) + s, BF16) for s in (own_u, own_d)],
        in_specs=[hbm, vmem, vmem],
        out_specs=[vmem] * 3 + [hbm] * 2,
        scratch_shapes=scratch,
        compiler_params=pltpu.CompilerParams(collective_id=1, has_side_effects=True, vmem_limit_bytes=VMEM_LIMIT),
    )(xa, mom_up, mom_down)
    return oa, ou, od


def update_kernel(scales, *refs):
    for k, scale in enumerate(scales):
        o, new, w = refs[3 * k:3 * k + 3]
        new_out, w_out, b_out = refs[9 + 3 * k:12 + 3 * k]
        new_out[...] = new[...]
        old = w[...]
        updated = old - LEARN_RATE * (scale * o[...].astype(F32) + WEIGHT_DECAY * old)
        w_out[...] = updated
        b_out[...] = updated.astype(BF16)


def update(group, orthos, moms, masters):
    args, outs, scales = [], [], []
    for o, new, w in zip(orthos, moms, masters):
        args += [o, new, w]
        outs += [jax.ShapeDtypeStruct(w.shape, F32)] * 2 + [jax.ShapeDtypeStruct(w.shape, BF16)]
        scales.append(0.2 * math.sqrt(max(group * w.shape[0], w.shape[1])))
    vmem = pl.BlockSpec(memory_space=pltpu.VMEM)
    return pl.pallas_call(
        functools.partial(update_kernel, scales), name="update", out_shape=outs,
        in_specs=[vmem] * 9, out_specs=[vmem] * 9,
    )(*args)


def solution(mesh):
    ax = mesh.axis_names[1]
    group = mesh.shape[ax]
    side = math.isqrt(group // 2)
    grad_spec = P(tuple(mesh.axis_names), None, None, None)
    row_spec = P(mesh.axis_names[0], ax, None)

    def step_local(*arrays):
        grads = [arrays[3 * k][0, 0] for k in range(3)]
        moms = [arrays[3 * k + 1][0] for k in range(3)]
        masters = [arrays[3 * k + 2][0] for k in range(3)]
        na, nu, nd, xa = reduce_and_gather(side, ax, grads, moms)
        oa, ou, od = orthogonalize(side, ax, xa, nu, nd)
        return tuple(r[None] for r in update(group, (oa, ou, od), (na, nu, nd), masters))

    return jax.shard_map(step_local, mesh=mesh, in_specs=(grad_spec, row_spec, row_spec) * 3,
                         out_specs=(row_spec,) * 9, check_vma=False)
```

```python
import functools
import math

import jax
import jax.numpy as jnp
from jax import lax
from jax.experimental import pallas as pl
from jax.experimental.pallas import tpu as pltpu
from jax.sharding import PartitionSpec as P

MOMENTUM = 0.95
LEARN_RATE = 0.25
WEIGHT_DECAY = 0.2
EPSILON = 1e-7
COEF_A = 3.4445
COEF_B = -4.7750
COEF_C = 2.0315
NS_STEPS = 5
F32 = jnp.float32
BF16 = jnp.bfloat16
MESH = pl.DeviceIdType.MESH
VMEM_LIMIT = 66_000_000
ATTN, UP, DOWN = MATRICES = range(3)
FIRST, SECOND = PAIR = range(2)
ALL = slice(None)
QUAD = range(4)


class Comm:
    def __init__(self, side, group, ax, mats, slots, local_sem, send_sem, recv_sem):
        self.side, self.group, self.ax, self.mats, self.slots = side, group, ax, mats, slots
        self.local_sem, self.send_sem, self.recv_sem = local_sem, send_sem, recv_sem
        me = lax.axis_index(ax)
        self.role = lax.rem(me, 4)
        self.c = lax.rem(me, 2)
        self.x = lax.rem(me // 2, side)
        self.y = me // (2 * side)
        self.peer = self.dev(self.y, self.x, 1 - self.c)
        self.pos = ((self.x, self.y), (self.y, self.x))
        self.keys, self.local_keys, self.sent, self.peer_only = {}, {}, {}, {}

    def dev(self, yy, xx, cc):
        return {self.ax: (lax.rem(yy, self.side) * self.side + lax.rem(xx, self.side)) * 2 + cc}

    def greet(self):
        barrier = pltpu.get_barrier_semaphore()
        pl.semaphore_signal(barrier, inc=1, device_id=self.peer, device_id_type=MESH)
        for k in range(1, self.side):
            pl.semaphore_signal(barrier, inc=1, device_id=self.dev(self.y + k, self.x, self.c), device_id_type=MESH)
            pl.semaphore_signal(barrier, inc=1, device_id=self.dev(self.y, self.x + k, self.c), device_id_type=MESH)
        return 2 * self.side - 1

    def to(self, along_x, step):
        step = step % self.side
        return self.dev(self.y, self.x + step, self.c) if along_x else self.dev(self.y + step, self.x, self.c)

    def remote(self, key, src, dst, target):
        k = self.keys.setdefault(key, len(self.keys))
        return pltpu.make_async_remote_copy(src, dst, self.send_sem.at[k], self.recv_sem.at[k],
                                            device_id=target, device_id_type=MESH)

    def local(self, key, src, dst):
        k = self.local_keys.setdefault(key, len(self.local_keys))
        return pltpu.make_async_copy(src, dst, self.local_sem.at[k])

    def start(self, make, *args):
        make(*args).start()
        self.sent[(make.__name__,) + args] = (make, args)

    def finish(self):
        for make, args in self.sent.values():
            make(*args).wait_send()

    def shift(self, p, k):
        return lax.rem(p + k, self.side)

    def quarter(self, m, f, h):
        q = self.mats[m]["own"].shape[-1] // 4
        return pl.ds((2 * f + h) * q, q)

    def half(self, m, f):
        q = self.mats[m]["own"].shape[-1] // 2
        return pl.ds(f * q, q)

    @staticmethod
    def lane1(f, k):
        return (ALL, k) if f == 0 else (k, ALL)

    @staticmethod
    def one(f, k, i):
        return (i, k) if f == 0 else (k, i)

    def pair_remote(self, m, f, k):
        idx = self.lane1(f, self.shift(self.pos[f][0], k))
        cols = self.half(m, f)
        mat = self.mats[m]
        return self.remote(("pair", m, f, k), mat["grad"].at[idx + (1 - self.c, ALL, cols)],
                           mat["peer"].at[idx + (ALL, cols)], self.peer)

    def pair_local(self, m, f, k):
        idx = self.lane1(f, self.shift(self.pos[f][0], k))
        cols = self.half(m, f)
        mat = self.mats[m]
        return self.local(("pair", m, f, k), mat["grad"].at[idx + (self.c, ALL, cols)],
                          mat["sum"].at[idx + (ALL, cols)])

    def pair_start(self, m):
        for k in (2, 1, self.side - 1, 0):
            for f in PAIR:
                self.start(self.pair_remote, m, f, k)
                self.pair_local(m, f, k).start()

    def pair_sum(self, m, f, k):
        self.pair_remote(m, f, k).wait_recv()
        self.pair_local(m, f, k).wait()
        kk = self.shift(self.pos[f][0], k)
        cols = self.half(m, f)
        total, other = self.mats[m]["sum"], self.mats[m]["peer"]

        @pl.loop(0, self.side)
        def _(i):
            idx = self.one(f, kk, i) + (ALL, cols)
            total[idx] = total[idx] + other[idx]

    def ring(self, m, f, phase, j):
        k, h, step = ((2, 1, 1), (2, 0, -1), (1, 0, 1), (-1, 1, -1), (1, 1, 1), (-1, 0, -1))[j]
        kk = self.shift(self.pos[f][phase], k % self.side)
        mat = self.mats[m]
        src = self.part(m, f, kk, h) if phase else mat["sum"].at[self.lane1(f, kk) + (ALL, self.quarter(m, f, h))]
        return self.remote(("ring", m, f, phase, j), src, mat[("ring1", "ring2")[phase]].at[f, j],
                           self.to((f == 0) == (phase == 0), step))

    def part(self, m, f, k, h):
        q = self.mats[m]["own"].shape[-1] // 4
        return self.mats[m]["line"].at[f, k, :, pl.ds(h * q, q)]

    def ring_add(self, m, f, phase, j, k, h):
        self.ring(m, f, phase, j).wait_recv()
        kk = self.shift(self.pos[f][phase], k % self.side)
        cols = self.quarter(m, f, h)
        mat = self.mats[m]
        if phase == 0:
            total = mat["sum"]

            @pl.loop(0, self.side)
            def _(i):
                idx = self.one(f, kk, i) + (ALL, cols)
                total[idx] = total[idx] + mat["ring1"][f, j, i]
        else:
            ref = self.part(m, f, kk, h)
            ref[...] = ref[...] + mat["ring2"][f, j]

    def rs_far(self, m):
        for f in PAIR:
            self.pair_sum(m, f, 2)
            self.start(self.ring, m, f, 0, 0)
            self.start(self.ring, m, f, 0, 1)

    def rs_near(self, m):
        for f in PAIR:
            self.pair_sum(m, f, 1)
            self.start(self.ring, m, f, 0, 2)
            self.pair_sum(m, f, self.side - 1)
            self.start(self.ring, m, f, 0, 3)

    def rs_own(self, m):
        for f in PAIR:
            self.pair_sum(m, f, 0)

    def pass_on(self, m, phase):
        for f in PAIR:
            self.ring_add(m, f, phase, 0, 1, 1)
            self.start(self.ring, m, f, phase, 4)
            self.ring_add(m, f, phase, 1, -1, 0)
            self.start(self.ring, m, f, phase, 5)

    def settle(self, m, phase):
        for f in PAIR:
            for h, pair in enumerate(((2, 5), (3, 4))):
                if phase:
                    for j in pair:
                        self.ring_add(m, f, phase, j, 0, h)
                    continue
                for j in pair:
                    self.ring(m, f, phase, j).wait_recv()
                self.line_up(m, f, h, pair)

    def line_up(self, m, f, h, pair):
        mat = self.mats[m]
        here = self.pos[f][0]
        left, right = pair

        @pl.loop(0, self.side)
        def _(i):
            held = mat["sum"][self.one(f, here, i) + (ALL, self.quarter(m, f, h))]
            self.part(m, f, i, h)[...] = held + mat["ring1"][f, left, i] + mat["ring1"][f, right, i]

    def turn(self, m):
        for f in PAIR:
            for j in QUAD:
                self.start(self.ring, m, f, SECOND, j)

    def norm_pair(self, m):
        ref = self.slots.at[m, 0, self.c]
        return self.remote(("norm", m), ref, ref, self.peer)

    def norm_line(self, m, level, k):
        ref = self.slots.at[m, level, self.x if level == 1 else self.y]
        return self.remote(("norm", m, level, k), ref, ref, self.to(level == 1, k))

    def momentum(self, m):
        mat = self.mats[m]
        for f in PAIR:
            cols = self.half(m, f)
            mat["new"][:, cols] = MOMENTUM * mat["mom"][:, cols] + mat["line"][f, self.pos[f][1]] / self.group

    def squares(self, m):
        mat = self.mats[m]
        rows, cols = mat["new"].shape
        acc = jnp.zeros((8, 128), F32)
        for i in range(0, rows, 8):
            for j in range(0, cols, 128):
                part = mat["new"][i:i + 8, j:j + 128]
                acc = acc + part * part
        self.slots[m, 0, self.c] = acc
        self.start(self.norm_pair, m)

    def norm_x(self, m):
        self.norm_pair(m).wait_recv()
        self.slots[m, 1, self.x] = self.slots[m, 0, 0] + self.slots[m, 0, 1]
        for k in range(1, self.side):
            self.start(self.norm_line, m, 1, k)

    def level_sum(self, m, level):
        for k in range(1, self.side):
            self.norm_line(m, level, k).wait_recv()
        acc = self.slots[m, level, 0]
        for k in range(1, self.side):
            acc = acc + self.slots[m, level, k]
        return acc

    def norm_y(self, m):
        self.slots[m, 2, self.y] = self.level_sum(m, 1)
        for k in range(1, self.side):
            self.start(self.norm_line, m, 2, k)

    def normalize(self, m):
        mat = self.mats[m]
        norm = jnp.sqrt(jnp.sum(self.level_sum(m, 2), axis=(0, 1), keepdims=True))
        mat["own"][...] = (mat["new"][...] / (norm + EPSILON)).astype(BF16)

    def along(self, f, phase):
        return (f == 0) != (phase == 0)

    def gpos(self, f, phase):
        return self.x if self.along(f, phase) else self.y

    def spot(self, m, f, phase, k, cols):
        if phase == 0:
            idx = (k, self.x) if f == 0 else (self.y, k)
        else:
            idx = self.lane1(f, k)
        return self.mats[m]["full"].at[idx + (self.c, ALL, cols)]

    def ag_own(self, m):
        return self.local(("own", m), self.mats[m]["own"], self.mats[m]["full"].at[self.y, self.x, self.c])

    def ag_send(self, m, f, phase, j):
        dst = self.spot(m, f, phase, self.gpos(f, phase), self.half(m, f))
        src = self.mats[m]["own"].at[:, self.half(m, f)] if phase == 0 else dst
        return self.remote(("send", m, f, phase, j), src, dst, self.to(self.along(f, phase), (1, -1)[j]))

    def ag_relay(self, m, f, phase, j):
        ref = self.spot(m, f, phase, self.shift(self.gpos(f, phase), (self.side - 1, 1)[j]), self.quarter(m, f, (1, 0)[j]))
        return self.remote(("relay", m, f, phase, j), ref, ref, self.to(self.along(f, phase), (1, -1)[j]))

    def ag_peer(self, m, f, k):
        ref = self.spot(m, f, 1, self.shift(self.gpos(f, 1), k), self.half(m, f))
        return self.remote(("peer", m, f, k), ref, ref, self.peer)

    def to_peer(self, m, f, k):
        self.peer_only[m, f, k] = True

        @pl.when(self.sends(m))
        def _():
            self.ag_peer(m, f, k).start()

    def sends(self, m):
        return self.role < 2 if m == 0 else self.role == 4 - m

    def needs(self, m):
        return self.role < 2 if m == 0 else self.role == 1 + m

    def ag_start(self, m):
        self.ag_own(m).start()
        for f in PAIR:
            for j in PAIR:
                self.start(self.ag_send, m, f, 0, j)

    def ag_forward(self, m, phase):
        for f in PAIR:
            for j in PAIR:
                self.ag_send(m, f, phase, j).wait_recv()
                self.start(self.ag_relay, m, f, phase, j)
                if phase == 1:
                    self.to_peer(m, f, (self.side - 1, 1)[j])

    def ag_turn(self, m):
        self.ag_own(m).wait()
        for f in PAIR:
            for j in PAIR:
                self.ag_relay(m, f, 0, j).wait_recv()
            for j in PAIR:
                self.start(self.ag_send, m, f, 1, j)
            self.to_peer(m, f, 0)

    def ag_end(self, m):
        for f in PAIR:
            for j in PAIR:
                self.ag_relay(m, f, 1, j).wait_recv()
            self.to_peer(m, f, 2)

    def ag_arrived(self, m):
        @pl.when(self.needs(m))
        def _():
            for f in PAIR:
                for k in range(self.side):
                    self.ag_peer(m, f, k).wait_recv()

    def ag_finish(self, m):
        @pl.when(self.sends(m))
        def _():
            for f in PAIR:
                for k in range(self.side):
                    self.ag_peer(m, f, k).wait_send()


def reduce_kernel(side, group, ax, ga, gu, gd, ma, na, lu, ld, xa,
                  sa, su, sd, pa, pu, pd, ra1, ru1, rd1, ra2, la, xra, xru, xrd, slots, local_sem, send_sem, recv_sem):
    mats = {ATTN: dict(grad=ga, mom=ma, new=na, full=xa, sum=sa, peer=pa, ring1=ra1, ring2=ra2, line=la, own=xra),
            UP: dict(grad=gu, line=lu, sum=su, peer=pu, ring1=ru1, own=xru),
            DOWN: dict(grad=gd, line=ld, sum=sd, peer=pd, ring1=rd1, own=xrd)}
    comm = Comm(side, group, ax, mats, slots, local_sem, send_sem, recv_sem)
    pl.semaphore_wait(pltpu.get_barrier_semaphore(), comm.greet())
    comm.pair_start(ATTN)
    comm.pair_start(UP)
    comm.pair_start(DOWN)
    comm.rs_far(ATTN)
    comm.rs_near(ATTN)
    comm.rs_own(ATTN)
    comm.pass_on(ATTN, FIRST)
    comm.rs_far(UP)
    comm.settle(ATTN, FIRST)
    comm.turn(ATTN)
    comm.rs_near(UP)
    comm.pass_on(ATTN, SECOND)
    comm.rs_own(UP)
    comm.pass_on(UP, FIRST)
    comm.settle(ATTN, SECOND)
    comm.momentum(ATTN)
    comm.squares(ATTN)
    comm.rs_far(DOWN)
    comm.norm_x(ATTN)
    comm.rs_near(DOWN)
    comm.norm_y(ATTN)
    comm.normalize(ATTN)
    comm.ag_start(ATTN)
    comm.settle(UP, FIRST)
    comm.rs_own(DOWN)
    comm.pass_on(DOWN, FIRST)
    comm.ag_forward(ATTN, FIRST)
    comm.ag_turn(ATTN)
    comm.settle(DOWN, FIRST)
    comm.ag_forward(ATTN, SECOND)
    comm.ag_end(ATTN)
    comm.ag_arrived(ATTN)
    comm.finish()
    comm.ag_finish(ATTN)


def line_shape(side, rows, cols):
    return 2, side, rows, cols // 2


def reduce_and_gather(side, ax, grads, moms):
    dma = pltpu.SemaphoreType.DMA
    vmem = pl.BlockSpec(memory_space=pltpu.VMEM)
    hbm = pl.BlockSpec(memory_space=pl.ANY)
    group = 2 * side * side
    shapes = [m.shape for m in moms]
    views = [g.reshape(side, side, 2, *s) for g, s in zip(grads, shapes)]
    attn = shapes[ATTN]
    scratch = [pltpu.VMEM((side, side) + each, F32) for each in shapes] * 2
    scratch += [pltpu.VMEM((2, 6, side, each[0], each[1] // 4), F32) for each in shapes]
    scratch += [pltpu.VMEM((2, 6, attn[0], attn[1] // 4), F32), pltpu.VMEM(line_shape(side, *attn), F32)]
    scratch += [pltpu.VMEM(each, BF16) for each in shapes]
    scratch += [pltpu.VMEM((2, 3, side, 8, 128), F32), dma((30,)), dma((130,)), dma((130,))]
    na, lu, ld, xa = pl.pallas_call(
        functools.partial(reduce_kernel, side, group, ax),
        name="reduce_gather",
        out_shape=[jax.ShapeDtypeStruct(attn, F32)]
        + [jax.ShapeDtypeStruct(line_shape(side, *each), F32) for each in shapes[1:]]
        + [jax.ShapeDtypeStruct((side, side, 2) + attn, BF16)],
        in_specs=[hbm] * 3 + [vmem],
        out_specs=[vmem] * 3 + [hbm],
        scratch_shapes=scratch,
        compiler_params=pltpu.CompilerParams(collective_id=0, has_side_effects=True, vmem_limit_bytes=VMEM_LIMIT),
    )(*views, moms[ATTN])
    return na, lu, ld, xa.reshape(group * shapes[0][0], shapes[0][1])


def ns_kernel(n, side, group, ax, xa, lu_in, ld_in, mu, md, oa_out, ou_out, od_out, nu, nd, xu, xd,
              X, A, B, stage, obuf, oa, ou, od, lu, ld, ru2, rd2, xru, xrd, slots,
              load_sem, asend, arecv, bsend, brecv, xsend, xrecv, osend, orecv, local_sem, send_sem, recv_sem):
    me = lax.axis_index(ax)
    role = lax.rem(me, 4)
    base = me - role
    mats = {UP: dict(mom=mu, new=nu, line=lu, ring2=ru2, full=xu, own=xru),
            DOWN: dict(mom=md, new=nd, line=ld, ring2=rd2, full=xd, own=xrd)}
    comm = Comm(side, group, ax, mats, slots, local_sem, send_sem, recv_sem)
    blk = n // 4
    half = n // 2

    def dev(k):
        return {ax: k}

    barrier = pltpu.get_barrier_semaphore()
    greeted = comm.greet()
    for step in range(1, 4):
        pl.semaphore_signal(barrier, inc=1, device_id=dev(base + lax.rem(role + step, 4)), device_id_type=MESH)
    pl.semaphore_wait(barrier, greeted + 3)
    lu[...] = lu_in[...]
    comm.turn(UP)
    ld[...] = ld_in[...]
    comm.turn(DOWN)
    steps = (
        ("0A0", (comm.pass_on, UP, SECOND), (comm.pass_on, DOWN, SECOND)),
        ("0A3", (comm.settle, UP, SECOND), (comm.momentum, UP), (comm.squares, UP)),
        ("0Q1", (comm.settle, DOWN, SECOND), (comm.momentum, DOWN), (comm.squares, DOWN)),
        ("0Q3", (comm.norm_x, UP), (comm.norm_x, DOWN)),
        ("0Y1", (comm.norm_y, UP), (comm.norm_y, DOWN)),
        ("0Y3", (comm.normalize, UP), (comm.ag_start, UP), (comm.normalize, DOWN), (comm.ag_start, DOWN)),
        ("1A2", (comm.ag_forward, UP, FIRST), (comm.ag_forward, DOWN, FIRST)),
        ("1Q1", (comm.ag_turn, UP), (comm.ag_turn, DOWN)),
        ("1Y2", (comm.ag_forward, UP, SECOND)),
        ("1Y3", (comm.ag_forward, DOWN, SECOND)),
        ("2A2", (comm.ag_end, UP)),
        ("2Q0", (comm.ag_end, DOWN)),
    )

    def run(calls):
        for call, *what in calls:
            call(*what)

    def tick(t, part, i):
        if isinstance(t, int):
            return
        for (when, where, block), *calls in steps:
            if where == part:
                go = jnp.logical_and(t == int(when), i == int(block))
                pl.when(go)(functools.partial(run, calls))

    def at(ref, i, j):
        return ref.at[pl.ds(pl.multiple_of(i * blk, blk), blk), pl.ds(pl.multiple_of(j * blk, blk), blk)]

    def rows(i, size=blk):
        return pl.ds(pl.multiple_of(i * size, size), size)

    def poly(a, q):
        return (COEF_B * a.astype(F32) + COEF_C * q.astype(BF16).astype(F32)).astype(BF16)

    def blend(x, y):
        return (COEF_A * x.astype(F32) + y.astype(BF16).astype(F32)).astype(BF16)

    def dot_nt(a, b):
        return lax.dot_general(a, b, (((1,), (1,)), ((), ())), preferred_element_type=F32)

    def dot(a, b):
        return jnp.dot(a, b, preferred_element_type=F32)

    @pl.when(role < 2)
    def _():
        c = role
        peer = dev(base + 1 - c)
        p_own, s_own = 3 * c, 1 + c
        p_peer, s_peer = 3 - 3 * c, 2 - c
        i1, j1 = 1 + 2 * c, 3 - 3 * c
        i2, j2 = 2 * c, 2 - c

        loads = [pltpu.make_async_copy(xa.at[rows(p)], X.at[0, rows(p)], load_sem.at[k])
                 for k, p in enumerate((p_own, s_own, p_peer, s_peer))]
        for cp in loads:
            cp.start()
        for cp in loads[:2]:
            cp.wait()

        def a_copy(k, i, j):
            return pltpu.make_async_remote_copy(at(A, i, j), at(A, i, j), asend.at[k], arecv.at[k],
                                                device_id=peer, device_id_type=MESH)

        a_blocks = ((p_own, p_own), (p_own, s_own), (s_own, p_own), (i1, j1), (j1, i1), (i2, j2), (j2, i2), (s_own, s_own))
        PP, PS, SP, C1, T1, C2, T2, SS = every = range(len(a_blocks))

        def a_send(k):
            a_copy(k, *a_blocks[k]).start()

        def a_wait(*ks):
            for k in ks:
                a_copy(k, *a_blocks[k]).wait_recv()

        mine = pl.ds(pl.multiple_of(half * c, half), half)

        def x_copy(nxt, j):
            ref = X.at[nxt, mine, pl.ds(pl.multiple_of(j * blk, blk), blk)]
            return pltpu.make_async_remote_copy(ref, ref, xsend.at[j], xrecv.at[j], device_id=peer, device_id_type=MESH)

        def b_copy(k):
            i, j = ((i1, j1), (i2, j2))[k]
            return pltpu.make_async_remote_copy(stage.at[k], at(B, j - 2 * (1 - c), i), bsend.at[k], brecv.at[k],
                                                device_id=peer, device_id_type=MESH)

        def gram(xt, i, j, mirror):
            v = dot_nt(xt[rows(i), :], xt[rows(j), :]).astype(BF16)
            at(A, i, j)[...] = v
            if mirror:
                at(A, j, i)[...] = v.T

        def col(j):
            return pl.ds(pl.multiple_of(j * blk, blk), blk)

        def a_step(t, cur):
            xt = X.at[cur]
            A[mine, col(p_own)] = dot_nt(xt[mine, :], xt[rows(p_own), :]).astype(BF16)
            at(A, p_own, s_own)[...] = at(A, s_own, p_own)[...].T

            @pl.when(t > 0)
            def _():
                for j in QUAD:
                    x_copy(cur, j).wait_recv()
            a_send(PP)
            a_send(SP)
            a_send(PS)
            tick(t, "A", 0)

            @pl.when(t == 0)
            def _():
                for cp in loads[2:]:
                    cp.wait()
            gram(xt, i1, j1, True)
            a_send(C1)
            a_send(T1)
            tick(t, "A", 1)
            gram(xt, i2, j2, True)
            a_send(C2)
            a_send(T2)
            tick(t, "A", 2)
            gram(xt, s_own, s_own, False)
            a_send(SS)
            tick(t, "A", 3)

        def sent(t, cur):
            for k in every:
                a_copy(k, *a_blocks[k]).wait_send()

            @pl.when(t > 0)
            def _():
                for j in QUAD:
                    x_copy(cur, j).wait_send()

        def q_block(i, j):
            v = poly(at(A, i, j)[...], dot(A[rows(i), :], A[:, col(j)]))
            at(B, i - 2 * c, j)[...] = v
            return v

        def q_step(t, cur):
            a_wait(C1, T1)
            q_block(p_own, p_own)
            tick(t, "Q", 0)
            a_wait(C2, T2, PP, PS, SP)
            stage[FIRST] = q_block(i1, j1).T
            b_copy(FIRST).start()
            tick(t, "Q", 1)
            a_wait(SS)
            stage[SECOND] = q_block(i2, j2).T
            b_copy(SECOND).start()
            tick(t, "Q", 2)
            B[:, col(s_own)] = poly(A[mine, col(s_own)], dot(A[mine, :], A[:, col(s_own)]))
            at(B, s_own - 2 * c, p_own)[...] = at(B, p_own - 2 * c, s_own)[...].T
            tick(t, "Q", 3)
            sent(t, cur)

        def y_step(t, cur, nxt):
            xt, xn = X.at[cur], X.at[nxt]
            for k in PAIR:
                b_copy(k).wait_recv()

            @pl.loop(0, 4)
            def _(j):
                xn[mine, col(j)] = blend(xt[mine, col(j)], dot(B[...], xt[:, col(j)]))
                x_copy(nxt, j).start()
                tick(t, "Y", j)
            for k in PAIR:
                b_copy(k).wait_send()

        for where, *calls in steps:
            if "L" in where:
                run(calls)
        last = NS_STEPS - 1

        @pl.loop(0, NS_STEPS)
        def _(t):
            cur = lax.rem(t, 2)
            a_step(t, cur)

            @pl.when(t < last)
            def _():
                q_step(t, cur)
                y_step(t, cur, 1 - cur)

        cur = last % 2
        a_wait(*every)
        sent(last, cur)
        own = oa.shape[0]
        ours = pl.ds(pl.multiple_of(own * (base + 2 * c), 2 * own), 2 * own)
        for j in QUAD:
            cols = pl.ds(j * blk, blk)
            B[0:2 * own, cols] = poly(A[ours, cols], dot(A[ours, :], A[:, cols]))

        def o_copy(k, target, j):
            cols = pl.ds(j * blk, blk)
            return pltpu.make_async_remote_copy(obuf.at[pl.ds(own * k, own), cols], oa.at[:, cols], osend.at[4 * k + j],
                                                orecv.at[j], device_id=dev(target), device_id_type=MESH)

        for j in QUAD:
            cols = pl.ds(j * blk, blk)
            obuf[0:2 * own, cols] = blend(X[cur, ours, cols], dot(B[0:2 * own, :], X[cur, :, cols]))

            @pl.when(c == 1)
            def _():
                o_copy(FIRST, base + 2, j).start()
                o_copy(SECOND, base + 3, j).start()

            @pl.when(c == 0)
            def _():
                o_copy(SECOND, base + 1, j).start()

        @pl.when(c == 1)
        def _():
            for j in QUAD:
                o_copy(FIRST, base + 2, j).wait_send()
                o_copy(SECOND, base + 3, j).wait_send()

        @pl.when(c == 0)
        def _():
            oa[...] = obuf[0:own, :]
            for j in QUAD:
                o_copy(SECOND, base + 1, j).wait_send()

    @pl.when(role >= 2)
    def _():
        for _, *calls in steps:
            run(calls)
        comm.ag_arrived(UP)
        comm.ag_arrived(DOWN)

        def load(full, place):
            own = full.shape[3]
            copies = [pltpu.make_async_copy(full.at[yy, xx, cc], place(pl.ds(((yy * side + xx) * 2 + cc) * own, own)),
                                            load_sem.at[(yy * side + xx) * 2 + cc])
                      for yy in range(side) for xx in range(side) for cc in PAIR]
            for cp in copies:
                cp.start()
            for cp in copies:
                cp.wait()

        @pl.when(role == 2)
        def _():
            load(xu, lambda rows_at: X.at[1, rows_at, pl.ds(0, half)])

            @pl.loop(0, 4)
            def _(i):
                for j in PAIR:
                    at(X.at[0], j, i)[...] = at(X.at[1], i, j)[...].T

        @pl.when(role == 3)
        def _():
            load(xd, lambda rows_at: X.at[0, rows_at])

        def a_step(cur):
            A[0:half, 0:blk] = dot_nt(X[cur, 0:half, :], X[cur, 0:blk, :]).astype(BF16)
            A[0:blk, blk:half] = A[blk:half, 0:blk].T
            A[blk:half, blk:half] = dot_nt(X[cur, blk:half, :], X[cur, blk:half, :]).astype(BF16)

        def q_step():
            B[0:half, 0:blk] = poly(A[0:half, 0:blk], dot(A[0:half, 0:half], A[0:half, 0:blk]))
            B[0:blk, blk:half] = B[blk:half, 0:blk].T
            B[blk:half, blk:half] = poly(A[blk:half, blk:half], dot(A[blk:half, 0:half], A[0:half, blk:half]))

        @pl.loop(0, NS_STEPS)
        def _(t):
            cur = lax.rem(t, 2)
            a_step(cur)

            @pl.when(jnp.logical_or(t < NS_STEPS - 1, role == 2))
            def _():
                q_step()

            @pl.when(t < NS_STEPS - 1)
            def _():
                @pl.loop(0, 4)
                def _(j):
                    cols = pl.ds(pl.multiple_of(j * blk, blk), blk)
                    y = dot(B[0:half, 0:half], X[cur, 0:half, cols])
                    X[1 - cur, 0:half, cols] = blend(X[cur, 0:half, cols], y)

        cur = (NS_STEPS - 1) % 2

        @pl.when(role == 2)
        def _():
            own = ou.shape[0]
            cols = pl.ds(pl.multiple_of(own * base, 4 * own), 4 * own)
            for i in PAIR:
                o = blend(X[cur, i * blk:(i + 1) * blk, cols], dot(B[i * blk:(i + 1) * blk, 0:half], X[cur, 0:half, cols]))
                obuf[0:4 * own, i * blk:(i + 1) * blk] = o.T

            def o_copy(k):
                return pltpu.make_async_remote_copy(obuf.at[pl.ds(own * k, own), pl.ds(0, half)], ou, osend.at[k], orecv.at[4],
                                                    device_id=dev(base + k), device_id_type=MESH)
            for k in (0, 1, 3):
                o_copy(k).start()
            ou[...] = obuf[2 * own:3 * own, 0:half]
            for k in (0, 1, 3):
                o_copy(k).wait_send()

        @pl.when(role == 3)
        def _():
            own = od.shape[0]
            mine = pl.ds(pl.multiple_of(own * base, 4 * own), 4 * own)
            for j in PAIR:
                cols = pl.ds(j * blk, blk)
                B[0:4 * own, cols] = poly(A[mine, cols], dot(A[mine, 0:half], A[0:half, cols]))
            for j in QUAD:
                cols = pl.ds(j * blk, blk)
                obuf[0:4 * own, cols] = blend(X[cur, mine, cols], dot(B[0:4 * own, 0:half], X[cur, 0:half, cols]))

            def o_copy(k):
                return pltpu.make_async_remote_copy(obuf.at[pl.ds(own * k, own)], od, osend.at[k], orecv.at[5],
                                                    device_id=dev(base + k), device_id_type=MESH)
            for k in (0, 1, 2):
                o_copy(k).start()
            od[...] = obuf[3 * own:4 * own, :]
            for k in (0, 1, 2):
                o_copy(k).wait_send()

    def arrived(o, k):
        pltpu.make_async_remote_copy(o, o, osend.at[k], orecv.at[k], device_id=dev(base), device_id_type=MESH).wait_recv()

    @pl.when(role != 3)
    def _():
        arrived(od, 5)
    od_out[...] = od[...]

    @pl.when(role != 2)
    def _():
        arrived(ou, 4)
    ou_out[...] = ou[...]

    @pl.when(role != 0)
    def _():
        for j in QUAD:
            arrived(oa.at[:, pl.ds(j * blk, blk)], j)
    oa_out[...] = oa[...]
    comm.finish()
    comm.ag_finish(UP)
    comm.ag_finish(DOWN)


def orthogonalize(side, ax, xa, line_up, line_down, mom_up, mom_down):
    n = xa.shape[1]
    blk = n // 4
    group = 2 * side * side
    dma = pltpu.SemaphoreType.DMA
    vmem = pl.BlockSpec(memory_space=pltpu.VMEM)
    hbm = pl.BlockSpec(memory_space=pl.ANY)
    own_a, own_u, own_d = (n // group, n), mom_up.shape, mom_down.shape
    scratch = [
        pltpu.VMEM((2, n, n), BF16),
        pltpu.VMEM((n, n), BF16),
        pltpu.VMEM((n // 2, n), BF16),
        pltpu.VMEM((2, blk, blk), BF16),
        pltpu.VMEM((4 * max(own_a[0], own_u[0]), n), BF16),
        pltpu.VMEM(own_a, BF16),
        pltpu.VMEM(own_u, BF16),
        pltpu.VMEM(own_d, BF16),
    ]
    scratch += [pltpu.VMEM(line_shape(side, *each), F32) for each in (own_u, own_d)]
    scratch += [pltpu.VMEM((2, 6, each[0], each[1] // 4), F32) for each in (own_u, own_d)]
    scratch += [pltpu.VMEM(own_u, BF16), pltpu.VMEM(own_d, BF16), pltpu.VMEM((3, 3, side, 8, 128), F32)]
    scratch += [dma((group,)), dma((8,)), dma((8,)), dma((2,)), dma((2,)), dma((4,)), dma((4,)), dma((8,)), dma((6,))]
    scratch += [dma((20,)), dma((110,)), dma((110,))]
    oa, ou, od, nu, nd, _, _ = pl.pallas_call(
        functools.partial(ns_kernel, n, side, group, ax),
        name="newton_schulz",
        out_shape=[jax.ShapeDtypeStruct(s, BF16) for s in (own_a, own_u, own_d)]
        + [jax.ShapeDtypeStruct(s, F32) for s in (own_u, own_d)]
        + [jax.ShapeDtypeStruct((side, side, 2) + s, BF16) for s in (own_u, own_d)],
        in_specs=[hbm] + [vmem] * 4,
        out_specs=[vmem] * 5 + [hbm] * 2,
        scratch_shapes=scratch,
        compiler_params=pltpu.CompilerParams(collective_id=1, has_side_effects=True, vmem_limit_bytes=VMEM_LIMIT),
    )(xa, line_up, line_down, mom_up, mom_down)
    return oa, ou, od, nu, nd


def update_kernel(scales, *refs):
    for k, scale in enumerate(scales):
        o, new, w = refs[3 * k:3 * k + 3]
        new_out, w_out, b_out = refs[9 + 3 * k:12 + 3 * k]
        new_out[...] = new[...]
        old = w[...]
        updated = old - LEARN_RATE * (scale * o[...].astype(F32) + WEIGHT_DECAY * old)
        w_out[...] = updated
        b_out[...] = updated.astype(BF16)


def update(group, orthos, moms, masters):
    args, outs, scales = [], [], []
    for o, new, w in zip(orthos, moms, masters):
        args += [o, new, w]
        outs += [jax.ShapeDtypeStruct(w.shape, F32)] * 2 + [jax.ShapeDtypeStruct(w.shape, BF16)]
        scales.append(0.2 * math.sqrt(max(group * w.shape[0], w.shape[1])))
    vmem = pl.BlockSpec(memory_space=pltpu.VMEM)
    return pl.pallas_call(
        functools.partial(update_kernel, scales), name="update", out_shape=outs,
        in_specs=[vmem] * 9, out_specs=[vmem] * 9,
    )(*args)


def solution(mesh):
    ax = mesh.axis_names[1]
    group = mesh.shape[ax]
    side = math.isqrt(group // 2)
    grad_spec = P(tuple(mesh.axis_names), None, None, None)
    row_spec = P(mesh.axis_names[0], ax, None)

    def step_local(*arrays):
        grads = [arrays[3 * k][0, 0] for k in range(3)]
        moms = [arrays[3 * k + 1][0] for k in range(3)]
        masters = [arrays[3 * k + 2][0] for k in range(3)]
        na, lu, ld, xa = reduce_and_gather(side, ax, grads, moms)
        oa, ou, od, nu, nd = orthogonalize(side, ax, xa, lu, ld, *moms[1:])
        return tuple(r[None] for r in update(group, (oa, ou, od), (na, nu, nd), masters))

    return jax.shard_map(step_local, mesh=mesh, in_specs=(grad_spec, row_spec, row_spec) * 3,
                         out_specs=(row_spec,) * 9, check_vma=False)
```
